32 devices in a mesh: gx: 2 (over y), gy: 4 (over z), gz: 4 (over x, core).
Axes of the slice: x: 2, y: 2, z: 4, core: 2. Of those that a mesh axis runs over, the one named last changes fastest.
Arguments:
- forcing: float32 [3, 16, 64, 512], P(None, 'gx', 'gy', 'gz'), may hold values from -8 to 8
- viscosity: float32 [16, 64, 512], P('gx', 'gy', 'gz'), may hold values from 0.001 to 1000
Outputs:
- solution: float32 [3, 16, 64, 512], P(None, 'gx', 'gy', 'gz')
- residual: float32 [3, 16, 64, 512], P(None, 'gx', 'gy', 'gz')
The draws below stay inside these ranges and needn't reach their ends.
All inputs are finite; a program needn't handle non-finite values.
Results may differ from the reference program's by a relative error of at most 0.00017.
Values sent between devices are 32-bit elements; how exact they have to be, the bound alone decides.
No kernel may reach another device: no remote copies, remote signals or barrier semaphores. Data moves between devices by JAX's collectives and lax.ppermute only.
A program may use at most 64 MiB of HBM per device.

```python
import math
import jax
import jax.numpy as jnp

ITERS = 3
CSWEEPS = 4
NX = 16
NY = 64
NZ = 512


def block_scale(stream_key, shape, split, smallest, high):
    gain = 1.0
    for dim, blocks in split:
        draws = jax.random.uniform(jax.random.fold_in(jax.random.fold_in(stream_key, 6), dim), (blocks,), jnp.float32, smallest / len(split), high / len(split))
        gain = gain * jnp.repeat(jnp.exp(draws), shape[dim] // blocks).reshape((-1,) + (1,) * (len(shape) - 1 - dim))
    return gain


def centred(stream_key, shape, width, reach, cuts=(), kind=jnp.bfloat16):
    gain = block_scale(stream_key, shape, cuts, -0.22, 0.18) if cuts else 1.0
    drawn = jax.random.normal(stream_key, shape, jnp.float32) * width * gain
    return jnp.minimum(jnp.maximum(drawn, -reach), reach).astype(kind)


def setup_inputs(seed: int = 0) -> dict:
    seeds = jax.random.split(jax.random.key(seed), 3)
    forcing = centred(seeds[0], (3, NX, NY, NZ), 1.0, 8.0, ((1, 2), (2, 4), (3, 4)), jnp.float32)
    viscosity = jnp.clip(jnp.exp(math.log(1000.0) - 13.815511 * jax.random.uniform(seeds[1], (NX, NY, NZ), jnp.float32) ** block_scale(seeds[1], (NX, NY, NZ), ((0, 2), (1, 4), (2, 4)), -0.2, 0.2)), 0.001, 1000.0)
    return dict(forcing=forcing, viscosity=viscosity)


reaction = 1.0
relaxation = 2.0 / 3.0
neighbours = ((1, 0, 0), (-1, 0, 0), (0, 1, 0), (0, -1, 0), (0, 0, 1), (0, 0, -1))


def window(padded, offset, extent):
    return padded[..., 1 + offset[0]:1 + offset[0] + extent[0], 1 + offset[1]:1 + offset[1] + extent[1], 1 + offset[2]:1 + offset[2] + extent[2]]


def viscous(values, padded_values, viscosity, padded_visc, mass_term, face_term):
    extent = viscosity.shape
    summed = mass_term * values
    for offset in neighbours:
        beside = window(padded_visc, offset, extent)
        across = window(padded_values, offset, extent)
        summed = summed + face_term * (viscosity + beside) * (values - across)
    return summed


def diagonal_of(viscosity, padded_visc, mass_term, face_term):
    summed = jnp.full(viscosity.shape, mass_term, jnp.float32)
    for offset in neighbours:
        summed = summed + face_term * (viscosity + window(padded_visc, offset, viscosity.shape))
    return summed


def restrict(values):
    extent = values.shape
    return values.reshape(extent[0], extent[1] // 2, 2, extent[2] // 2, 2, extent[3] // 2, 2).sum(axis=(2, 4, 6))


def prolong(values):
    return jnp.repeat(jnp.repeat(jnp.repeat(values, 2, axis=1), 2, axis=2), 2, axis=3)


def coarsen(viscosity):
    extent = viscosity.shape
    return viscosity.reshape(extent[0] // 2, 2, extent[1] // 2, 2, extent[2] // 2, 2).mean(axis=(1, 3, 5))


def sweeps(coarse_rhs, diagonal, applier):
    correction = relaxation * coarse_rhs / diagonal
    for counter in range(CSWEEPS - 1):
        correction = correction + relaxation * (coarse_rhs - applier(correction)) / diagonal
    return correction


def pad_all(values):
    return jnp.pad(values, ((0, 0), (1, 1), (1, 1), (1, 1)))


def reference(forcing, viscosity):
    padded_visc = jnp.pad(viscosity, 1)
    fine_diag = diagonal_of(viscosity, padded_visc, reaction, 0.5)
    coarse_visc = coarsen(viscosity)
    coarse_pad = jnp.pad(coarse_visc, 1)
    coarse_diag = diagonal_of(coarse_visc, coarse_pad, 8.0 * reaction, 2.0)

    def fine_apply(values):
        return viscous(values, pad_all(values), viscosity, padded_visc, reaction, 0.5)

    def coarse_apply(values):
        return viscous(values, pad_all(values), coarse_visc, coarse_pad, 8.0 * reaction, 2.0)

    def precondition(residual):
        smoothed = relaxation * residual / fine_diag
        defect = residual - fine_apply(smoothed)
        correction = sweeps(restrict(defect), coarse_diag, coarse_apply)
        smoothed = smoothed + prolong(correction)
        return smoothed + relaxation * (residual - fine_apply(smoothed)) / fine_diag

    solution = jnp.zeros_like(forcing)
    residual = forcing
    precond = precondition(residual)
    product = jnp.sum(residual * precond)
    direction = precond
    for iteration in range(ITERS):
        applied = fine_apply(direction)
        alpha_step = product / jnp.sum(direction * applied)
        solution = solution + alpha_step * direction
        residual = residual - alpha_step * applied
        if iteration + 1 < ITERS:
            precond = precondition(residual)
            product_next = jnp.sum(residual * precond)
            direction = precond + (product_next / product) * direction
            product = product_next
    return solution, residual
```

```python
import functools
import jax
import jax.numpy as jnp
from jax import lax
from jax.experimental import pallas as pl
from jax.experimental.pallas import tpu as pltpu
from jax.sharding import PartitionSpec as P

ITERS = 3
CSWEEPS = 4
REACTION = 1.0
RELAX = 2.0 / 3.0

STEP = 2 * (CSWEEPS - 1) + 4
HALO = ITERS * STEP
CHUNK = 16


def lane_iota(shape):
    return lax.broadcasted_iota(jnp.int32, shape, len(shape) - 1)


def sub_iota(shape):
    return lax.broadcasted_iota(jnp.int32, shape, len(shape) - 2)


def roll(v, shift, dim):
    size = v.shape[dim]
    return pltpu.roll(v, shift % size, dim)


def swap_blocks(v, count, width):
    sub, lane = sub_iota(v.shape), lane_iota(v.shape)
    step = 1
    while step < count:
        low = (sub // step) % 2 == 1
        high = (lane // (step * width)) % 2 == 1
        rows, lanes = v.ndim - 2, v.ndim - 1
        from_left = roll(roll(v, step, rows), -step * width, lanes)
        from_right = roll(roll(v, -step, rows), step * width, lanes)
        v = jnp.where(low == high, v, jnp.where(low, from_left, from_right))
        step *= 2
    return v


def chunked(lo, hi, n, body):
    n = min(n, hi - lo)
    count = -(-(hi - lo) // n)
    if count == 1:
        body(lo, n)
        return

    @pl.loop(0, count)
    def _(i):
        body(jnp.minimum(lo + i * n, hi - n), n)


class Sizes:
    def __init__(self, mesh, comps, xl, yl, zl):
        self.gx, self.gy, self.gz = (mesh[a] for a in ("gx", "gy", "gz"))
        self.comps, self.xl, self.yl, self.zl = comps, xl, yl, zl
        self.group = self.gx * self.gy
        self.planes = zl // self.gx
        self.rows = self.gx * xl // 2
        self.width = self.gy * yl
        self.lanes = xl * yl
        self.window = self.planes + 2 * HALO
        self.hops = []
        left = HALO
        while left > 0:
            self.hops.append(min(left, self.planes))
            left -= self.planes
        assert comps <= self.gy and xl == 2 * self.gy
        assert zl % (2 * self.gx) == 0 and 2 * self.width == self.lanes


def slab_of(sz, i):
    z, k = divmod(i, sz.gx)
    return (k if z % 2 == 0 else sz.gx - 1 - k) * sz.gz + z


def to_slab(sz, x, shift):
    n = sz.gx * sz.gz
    perm = [(slab_of(sz, i), slab_of(sz, i + shift)) for i in range(n) if 0 <= i + shift < n]
    return lax.ppermute(x, ("gx", "gz"), perm)


def x_order(sz):
    return list(range(0, sz.xl, 2)) + list(range(1, sz.xl, 2))


def part_of(sz, half):
    odd = lax.axis_index("gz") % 2
    return jnp.where(odd == 1, sz.gx - 1 - half, half)


def pack_kernel(sz, f_ref, v_ref, out_ref):
    def turned(at):
        return jnp.concatenate([at(x) for x in x_order(sz)], axis=0).T

    visc = turned(lambda x: v_ref[x])
    zero = jnp.zeros((sz.planes, sz.lanes), jnp.float32)
    for c in range(sz.gy):
        field = turned(lambda x: f_ref[c, x]) if c < sz.comps else None
        for half in range(sz.gx):
            dest = part_of(sz, half) * sz.gy + c
            cut = slice(half * sz.planes, (half + 1) * sz.planes)
            out_ref[dest, 0] = zero if field is None else field[cut]
            out_ref[dest, 1] = zero if field is None else visc[cut]


def planes_kernel(sz, in_ref, main_ref, *rest):
    edges, scr = rest[:-1], rest[-1]
    for a in range(2):
        for src in range(sz.group):
            scr[pl.ds(src, sz.planes, stride=sz.group), :] = in_ref[src, a]

        def body(p, n):
            rows = pl.multiple_of(p * sz.group, 8)
            v = scr[pl.ds(rows, n * sz.group), :].reshape(n, sz.group, sz.lanes)
            main_ref[a, pl.ds(p, n)] = swap_blocks(v, sz.gy, sz.yl)

        chunked(0, sz.planes, CHUNK, body)
        k = 0
        for count in sz.hops:
            if count < sz.planes:
                edges[k][a] = main_ref[a, 0:count]
                edges[k + 1][a] = main_ref[a, sz.planes - count : sz.planes]
                k += 2


def basis_kernel(sz, *refs):
    nh = len(sz.hops)
    main_ref, halos = refs[0], refs[1 : 1 + 2 * nh]
    u_out, rho_out, gram_out = refs[1 + 2 * nh : 4 + 2 * nh]
    it = iter(refs[4 + 2 * nh :])
    visc, cin, cout, cyp, cym, mass, cz, od = (next(it) for _ in range(8))
    cv, ccx, ccyp, ccym, cmass, ccz, cod, rhs, c0, c1 = (next(it) for _ in range(10))
    sm, sm2 = next(it), next(it)
    rhos = [next(it) for _ in range(ITERS + 1)]
    us = [next(it) for _ in range(ITERS)]

    H, N, W = HALO, sz.planes, sz.window
    for a, ref in ((0, rhos[0]), (1, visc)):
        ref[H : H + N] = main_ref[a]
        at_lo, at_hi = H, H + N
        for j, count in enumerate(sz.hops):
            ref[at_lo - count : at_lo] = halos[2 * j][a]
            ref[at_hi : at_hi + count] = halos[2 * j + 1][a]
            at_lo, at_hi = at_lo - count, at_hi + count

    plane = (1, sz.rows, sz.lanes)
    lane, sub = lane_iota(plane), sub_iota(plane)
    upper = lane >= sz.width
    y = lane % sz.width
    half_y = sz.width // 2

    def x_other(swapped):
        return jnp.where(upper, roll(swapped, -1, 1), roll(swapped, 1, 1))

    edge_out = (upper & (sub == sz.rows - 1)) | (~upper & (sub == 0))
    edge_yp, edge_ym = y == sz.width - 1, y == 0

    def split(total, edge):
        return jnp.where(edge, 0.0, total)

    def faces_z(ref, p, n, term):
        a, b = ref[pl.ds(p, n)], ref[pl.ds(p + 1, n)]
        return jnp.where((a > 0) & (b > 0), term * (a + b), 0.0)

    def fine_faces(p, n):
        cz[pl.ds(p, n)] = faces_z(visc, p, n, 0.5)

    chunked(0, W - 1, CHUNK, fine_faces)

    def fine_coeffs(p, n):
        v = visc[pl.ds(p, n)]
        before, after = visc[pl.ds(p - 1, n)], visc[pl.ds(p + 1, n)]
        swapped = roll(v, sz.width, 2)
        half = 0.5 * v
        inner = half + 0.5 * swapped
        outer = jnp.where(edge_out, 0.0, half + 0.5 * x_other(swapped))
        yp = jnp.where(edge_yp, 0.0, half + 0.5 * roll(v, -1, 2))
        ym = jnp.where(edge_ym, 0.0, half + 0.5 * roll(v, 1, 2))
        m = REACTION + jnp.where(edge_out, half, 0.0) + jnp.where(edge_yp | edge_ym, half, 0.0)
        m = m + jnp.where(before > 0, 0.0, half) + jnp.where(after > 0, 0.0, half)
        cin[pl.ds(p, n)] = inner
        cout[pl.ds(p, n)] = outer
        cyp[pl.ds(p, n)] = yp
        cym[pl.ds(p, n)] = ym
        mass[pl.ds(p, n)] = m
        od[pl.ds(p, n)] = RELAX / (m + inner + outer + yp + ym + cz[pl.ds(p - 1, n)] + cz[pl.ds(p, n)])

    chunked(1, W - 1, CHUNK, fine_coeffs)

    def gather_block(fine, n):
        t = fine.reshape(n, 2, sz.rows, sz.lanes)
        t = t[:, 0] + t[:, 1]
        t = t + roll(t, sz.width, 2)
        return t + jnp.where(lane % 2 == 0, roll(t, -1, 2), roll(t, 1, 2))

    def coarse_visc(p, n):
        cv[pl.ds(p, n)] = 0.125 * gather_block(visc[pl.ds(2 * p, 2 * n)], n)

    chunked(0, W // 2, CHUNK // 2, coarse_visc)

    def coarse_faces(p, n):
        ccz[pl.ds(p, n)] = faces_z(cv, p, n, 2.0)

    chunked(0, W // 2 - 1, CHUNK, coarse_faces)
    cedge_yp, cedge_ym = y >= sz.width - 2, y < 2

    def coarse_coeffs(p, n):
        v = cv[pl.ds(p, n)]
        before, after = cv[pl.ds(p - 1, n)], cv[pl.ds(p + 1, n)]
        twice = 2.0 * v
        xp = jnp.where(sub == sz.rows - 1, 0.0, twice + 2.0 * roll(v, -1, 1))
        yp = jnp.where(cedge_yp, 0.0, twice + 2.0 * roll(v, -2, 2))
        ym = jnp.where(cedge_ym, 0.0, twice + 2.0 * roll(v, 2, 2))
        m = 8.0 * REACTION + jnp.where(sub == 0, twice, 0.0) + jnp.where(sub == sz.rows - 1, twice, 0.0)
        m = m + jnp.where(cedge_yp, twice, 0.0) + jnp.where(cedge_ym, twice, 0.0)
        m = m + jnp.where(before > 0, 0.0, twice) + jnp.where(after > 0, 0.0, twice)
        ccx[pl.ds(p, n)] = xp
        ccyp[pl.ds(p, n)] = yp
        ccym[pl.ds(p, n)] = ym
        cmass[pl.ds(p, n)] = m
        cod[pl.ds(p, n)] = RELAX / (m + xp + roll(xp, 1, 1) + yp + ym + ccz[pl.ds(p - 1, n)] + ccz[pl.ds(p, n)])

    chunked(1, W // 2 - 1, CHUNK, coarse_coeffs)

    def fine_apply(ref, p, n):
        ext = ref[pl.ds(p - 1, n + 2)]
        v = ext[1 : n + 1]
        flux = cz[pl.ds(p - 1, n + 1)] * (ext[: n + 1] - ext[1:])
        swapped = roll(v, sz.width, 2)
        out = mass[pl.ds(p, n)] * v + (flux[1:] - flux[:n])
        out = out + cyp[pl.ds(p, n)] * (v - roll(v, -1, 2)) + cym[pl.ds(p, n)] * (v - roll(v, 1, 2))
        return out + cin[pl.ds(p, n)] * (v - swapped) + cout[pl.ds(p, n)] * (v - x_other(swapped))

    def coarse_apply(ref, p, n):
        ext = ref[pl.ds(p - 1, n + 2)]
        v = ext[1 : n + 1]
        flux = ccz[pl.ds(p - 1, n + 1)] * (ext[: n + 1] - ext[1:])
        fx = ccx[pl.ds(p, n)] * (v - roll(v, -1, 1))
        out = cmass[pl.ds(p, n)] * v + (flux[1:] - flux[:n]) + (fx - roll(fx, 1, 1))
        return out + ccyp[pl.ds(p, n)] * (v - roll(v, -2, 2)) + ccym[pl.ds(p, n)] * (v - roll(v, 2, 2))

    def spread(reach, n, body, unit=1):
        chunked((H - reach) // unit, (H + N + reach) // unit, n, body)

    for k in range(ITERS):
        reach = HALO - 1 - k * STEP
        rho, rho_next, u = rhos[k], rhos[k + 1], us[k]

        def smooth(p, n):
            sm[pl.ds(p, n)] = od[pl.ds(p, n)] * rho[pl.ds(p, n)]

        spread(reach, CHUNK, smooth)

        def restricted(p, n):
            defect = rho[pl.ds(2 * p, 2 * n)] - fine_apply(sm, 2 * p, 2 * n)
            b = gather_block(defect, n)
            rhs[pl.ds(p, n)] = b
            c0[pl.ds(p, n)] = cod[pl.ds(p, n)] * b

        spread(reach - 1, CHUNK // 2, restricted, 2)
        old, new = c0, c1
        for sweep in range(1, CSWEEPS):

            def relax(p, n):
                at = pl.ds(p, n)
                new[at] = old[at] + cod[at] * (rhs[at] - coarse_apply(old, p, n))

            spread(reach - 1 - 2 * sweep, CHUNK, relax, 2)
            old, new = new, old
        reach = reach - 1 - 2 * (CSWEEPS - 1)

        def prolonged(p, n):
            c = old[pl.ds(p, n)]
            fine = jnp.stack([c, c], axis=1).reshape(2 * n, sz.rows, sz.lanes)
            sm2[pl.ds(2 * p, 2 * n)] = sm[pl.ds(2 * p, 2 * n)] + fine

        spread(reach, CHUNK // 2, prolonged, 2)

        def smoothed(p, n):
            at = pl.ds(p, n)
            u[at] = sm2[at] + od[at] * (rho[at] - fine_apply(sm2, p, n))

        spread(reach - 1, CHUNK, smoothed)

        def descend(p, n):
            rho_next[pl.ds(p, n)] = rho[pl.ds(p, n)] - fine_apply(u, p, n)

        spread(reach - 2, CHUNK, descend)

    pairs = [(j, k) for j in range(ITERS + 1) for k in range(ITERS)]

    def products(i, sums):
        p = H + i
        rv = [r[p] for r in rhos]
        uv = [u[p] for u in us]
        for k in range(ITERS):
            u_out[k, i] = uv[k]
            rho_out[k, i] = rv[k + 1]
        return tuple(s + rv[j] * uv[k] for s, (j, k) in zip(sums, pairs))

    zero = jnp.zeros((sz.rows, sz.lanes), jnp.float32)
    sums = lax.fori_loop(0, N, products, (zero,) * len(pairs), unroll=4)
    wide = -(-len(pairs) // 8) * 8
    rows = [jnp.sum(s, axis=0, keepdims=True) for s in sums]
    rows = jnp.concatenate(rows + [jnp.zeros((wide - len(rows), sz.lanes), jnp.float32)], axis=0)
    total = jnp.broadcast_to(jnp.sum(rows, axis=1, keepdims=True), rows.shape)
    line = jnp.sum(jnp.where(sub_iota(rows.shape) == lane_iota(rows.shape), total, 0.0), axis=0, keepdims=True)
    gram_out[...] = jnp.broadcast_to(line[None], gram_out.shape)


def combine_kernel(sz, gram_ref, main_ref, u_ref, rho_ref, out_ref, scr):
    line = jnp.sum(gram_ref[...], axis=0)
    lane = lane_iota(line.shape)

    def entry(j, k):
        picked = jnp.where(lane == j * ITERS + k, line, 0.0)
        return jnp.broadcast_to(jnp.sum(picked, axis=1, keepdims=True), line.shape)

    g = [[entry(j, k) for k in range(ITERS)] for j in range(ITERS + 1)]
    zero = jnp.zeros_like(line)
    one = jnp.ones_like(line)

    def form(left, right, matrix):
        total = zero
        for j, a in enumerate(left):
            for k, b in enumerate(right):
                total = total + a * b * matrix(j, k)
        return total

    res = [one]
    direction = [one]
    sol = [zero] * ITERS
    product = g[0][0]
    for i in range(ITERS):
        alpha = product / form(direction, direction, lambda j, k: g[k][j] - g[k + 1][j])
        for k, b in enumerate(direction):
            sol[k] = sol[k] + alpha * b
        res = res + [zero]
        for k, b in enumerate(direction):
            res[k] = res[k] - alpha * b
            res[k + 1] = res[k + 1] + alpha * b
        if i + 1 < ITERS:
            following = form(res, res, lambda j, k: g[j][k])
            beta = following / product
            direction = [a + beta * b for a, b in zip(res, direction + [zero])]
            product = following

    sol = [s.reshape(1, 1, sz.lanes) for s in sol]
    res = [s.reshape(1, 1, sz.lanes) for s in res]

    for a in range(2):

        def body(p, n):
            at = pl.ds(p, n)
            if a == 0:
                v = sum(sol[k] * u_ref[k, at] for k in range(ITERS))
            else:
                v = res[0] * main_ref[0, at] + sum(res[k + 1] * rho_ref[k, at] for k in range(ITERS))
            v = swap_blocks(v, sz.gy, sz.yl)
            rows = pl.multiple_of(p * sz.group, 8)
            scr[pl.ds(rows, n * sz.group), :] = v.reshape(n * sz.group, sz.lanes)

        chunked(0, sz.planes, CHUNK, body)
        for dest in range(sz.group):
            out_ref[dest, a] = scr[pl.ds(dest, sz.planes, stride=sz.group), :]


def unpack_kernel(sz, in_ref, sol_ref, res_ref):
    for a, out in ((0, sol_ref), (1, res_ref)):
        for c in range(sz.comps):
            halves = [in_ref[part_of(sz, half) * sz.gy + c, a] for half in range(sz.gx)]
            turned = jnp.concatenate(halves, axis=0).T
            for i, x in enumerate(x_order(sz)):
                out[c, x] = turned[i * sz.yl : (i + 1) * sz.yl]


def vmem(count):
    return [pl.BlockSpec(memory_space=pltpu.VMEM)] * count


def call(kernel, sz, ins, outs, scratch=(), name=None):
    outs = [jax.ShapeDtypeStruct(s, jnp.float32) for s in outs]
    return pl.pallas_call(
        functools.partial(kernel, sz),
        in_specs=vmem(len(ins)),
        out_specs=vmem(len(outs)),
        out_shape=outs,
        scratch_shapes=[pltpu.VMEM(s, jnp.float32) for s in scratch],
        compiler_params=pltpu.CompilerParams(vmem_limit_bytes=56 * 2**20),
        name=name,
    )(*ins)


def shards(mesh, forcing, viscosity):
    comps, xl, yl, zl = forcing.shape
    sz = Sizes(mesh, comps, xl, yl, zl)
    N, W = sz.planes, sz.window
    plane = (sz.rows, sz.lanes)
    group_shape = (sz.group, 2, N, sz.lanes)
    (packed,) = call(pack_kernel, sz, [forcing, viscosity], [group_shape], name="pack")
    packed = lax.all_to_all(packed, ("gx", "gy"), 0, 0)
    edge_shapes = [(2, c) + plane for c in sz.hops if c < N for _ in range(2)]
    main, *edges = call(
        planes_kernel, sz, [packed], [(2, N) + plane] + edge_shapes, [(N * sz.group, sz.lanes)], name="planes"
    )
    halos = []
    for j, count in enumerate(sz.hops):
        first, last = (edges.pop(0), edges.pop(0)) if count < N else (main, main)
        halos += [to_slab(sz, last, j + 1), to_slab(sz, first, -(j + 1))]
    devices = sz.group * sz.gz
    fine, coarse = (W,) + plane, (W // 2,) + plane
    u, rho, gram = call(
        basis_kernel,
        sz,
        [main] + halos,
        [(ITERS, N) + plane, (ITERS, N) + plane, (devices, 1, sz.lanes)],
        [fine] * 8 + [coarse] * 10 + [fine] * (2 + 2 * ITERS + 1),
        name="basis",
    )
    gram = lax.all_to_all(gram, ("gx", "gy", "gz"), 0, 0)
    (mixed,) = call(
        combine_kernel, sz, [gram, main, u, rho], [group_shape], [(N * sz.group, sz.lanes)], name="combine"
    )
    mixed = lax.all_to_all(mixed, ("gx", "gy"), 0, 0)
    return tuple(call(unpack_kernel, sz, [mixed], [forcing.shape, forcing.shape], name="unpack"))


def solution(mesh):
    spec = P(None, "gx", "gy", "gz")
    return jax.shard_map(
        functools.partial(shards, dict(mesh.shape)),
        mesh=mesh,
        in_specs=(spec, P("gx", "gy", "gz")),
        out_specs=(spec, spec),
        check_vma=False,
    )
```

```python
import functools
import math
import jax
import jax.numpy as jnp
from jax import lax
from jax.experimental import pallas as pl
from jax.experimental.pallas import tpu as pltpu
from jax.sharding import PartitionSpec as P

ITERS = 3
CSWEEPS = 4
REACTION = 1.0
RELAX = 2.0 / 3.0

STEP = 2 * (CSWEEPS - 1) + 4
HALO = ITERS * STEP
BLOCK_ROWS = 1024


def lane_iota(shape):
    return lax.broadcasted_iota(jnp.int32, shape, len(shape) - 1)


def sub_iota(shape):
    return lax.broadcasted_iota(jnp.int32, shape, len(shape) - 2)


def roll(v, shift, dim):
    size = v.shape[dim]
    return pltpu.roll(v, shift % size, dim)


def swap_blocks(v, count, width):
    sub, lane = sub_iota(v.shape), lane_iota(v.shape)
    step = 1
    while step < count:
        low = (sub // step) % 2 == 1
        high = (lane // (step * width)) % 2 == 1
        rows, lanes = v.ndim - 2, v.ndim - 1
        from_left = roll(roll(v, step, rows), -step * width, lanes)
        from_right = roll(roll(v, -step, rows), step * width, lanes)
        v = jnp.where(low == high, v, jnp.where(low, from_left, from_right))
        step *= 2
    return v


def chunked(lo, hi, n, body):
    n = min(n, hi - lo)
    count = -(-(hi - lo) // n)
    if count == 1:
        body(lo, n)
        return

    @pl.loop(0, count)
    def _(i):
        body(jnp.minimum(lo + i * n, hi - n), n)


class Sizes:
    def __init__(self, mesh, comps, xl, yl, zl):
        self.gx, self.gy, self.gz = (mesh[a] for a in ("gx", "gy", "gz"))
        self.comps, self.xl, self.yl, self.zl = comps, xl, yl, zl
        self.group = self.gx * self.gy
        self.planes = zl // self.gx
        self.rows = self.gx * xl // 2
        self.width = self.gy * yl
        self.lanes = xl * yl
        self.window = self.planes + 2 * HALO
        self.chunk = max(2, BLOCK_ROWS // self.rows)
        self.hops = []
        left = HALO
        while left > 0:
            self.hops.append(min(left, self.planes))
            left -= self.planes
        assert comps <= self.gy and xl == 2 * self.gy
        assert zl % (2 * self.gx) == 0 and 2 * self.width == self.lanes


def slab_of(sz, i):
    z, k = divmod(i, sz.gx)
    return (k if z % 2 == 0 else sz.gx - 1 - k) * sz.gz + z


def to_slab(sz, x, shift):
    n = sz.gx * sz.gz
    perm = [(slab_of(sz, i), slab_of(sz, i + shift)) for i in range(n) if 0 <= i + shift < n]
    return lax.ppermute(x, ("gx", "gz"), perm)


def x_order(sz):
    return list(range(0, sz.xl, 2)) + list(range(1, sz.xl, 2))


def part_of(sz, half):
    odd = lax.axis_index("gz") % 2
    return jnp.where(odd == 1, sz.gx - 1 - half, half)


def pack_kernel(sz, f_ref, v_ref, out_ref):
    def turned(at):
        return jnp.concatenate([at(x) for x in x_order(sz)], axis=0).T

    visc = turned(lambda x: v_ref[x])
    zero = jnp.zeros((sz.planes, sz.lanes), jnp.float32)
    for c in range(sz.gy):
        field = turned(lambda x: f_ref[c, x]) if c < sz.comps else None
        for half in range(sz.gx):
            dest = part_of(sz, half) * sz.gy + c
            cut = slice(half * sz.planes, (half + 1) * sz.planes)
            out_ref[dest, 0] = zero if field is None else field[cut]
            out_ref[dest, 1] = zero if field is None else visc[cut]


def planes_kernel(sz, in_ref, main_ref, *rest):
    edges, scr = rest[:-1], rest[-1]
    for a in range(2):
        for src in range(sz.group):
            scr[pl.ds(src, sz.planes, stride=sz.group), :] = in_ref[src, a]

        def body(p, n):
            rows = pl.multiple_of(p * sz.group, 8)
            v = scr[pl.ds(rows, n * sz.group), :].reshape(n, sz.group, sz.lanes)
            main_ref[a, pl.ds(p, n)] = swap_blocks(v, sz.gy, sz.yl)

        chunked(0, sz.planes, sz.chunk, body)
        k = 0
        for count in sz.hops:
            if count < sz.planes:
                edges[k][a] = main_ref[a, 0:count]
                edges[k + 1][a] = main_ref[a, sz.planes - count : sz.planes]
                k += 2


def basis_kernel(sz, *refs):
    nh = len(sz.hops)
    main_ref, halos = refs[0], refs[1 : 1 + 2 * nh]
    u_out, rho_out, gram_out = refs[1 + 2 * nh : 4 + 2 * nh]
    it = iter(refs[4 + 2 * nh :])
    visc, cin, cout, cyp, cym, mass, cz, od = (next(it) for _ in range(8))
    cv, ccx, ccyp, ccym, cmass, ccz, cod, rhs, c0, c1 = (next(it) for _ in range(10))
    sm, sm2 = next(it), next(it)
    rhos = [next(it) for _ in range(ITERS + 1)]
    us = [next(it) for _ in range(ITERS)]

    H, N, W, C = HALO, sz.planes, sz.window, sz.chunk
    for a, ref in ((0, rhos[0]), (1, visc)):
        ref[H : H + N] = main_ref[a]
        at_lo, at_hi = H, H + N
        for j, count in enumerate(sz.hops):
            ref[at_lo - count : at_lo] = halos[2 * j][a]
            ref[at_hi : at_hi + count] = halos[2 * j + 1][a]
            at_lo, at_hi = at_lo - count, at_hi + count

    plane = (1, sz.rows, sz.lanes)
    lane, sub = lane_iota(plane), sub_iota(plane)
    upper = lane >= sz.width
    y = lane % sz.width
    half_y = sz.width // 2

    def x_other(swapped):
        return jnp.where(upper, roll(swapped, -1, 1), roll(swapped, 1, 1))

    edge_out = (upper & (sub == sz.rows - 1)) | (~upper & (sub == 0))
    edge_yp, edge_ym = y == sz.width - 1, y == 0

    def split(total, edge):
        return jnp.where(edge, 0.0, total)

    def faces_z(ref, p, n, term):
        a, b = ref[pl.ds(p, n)], ref[pl.ds(p + 1, n)]
        return jnp.where((a > 0) & (b > 0), term * (a + b), 0.0)

    def fine_faces(p, n):
        cz[pl.ds(p, n)] = faces_z(visc, p, n, 0.5)

    chunked(0, W - 1, C, fine_faces)

    def fine_coeffs(p, n):
        v = visc[pl.ds(p, n)]
        before, after = visc[pl.ds(p - 1, n)], visc[pl.ds(p + 1, n)]
        swapped = roll(v, sz.width, 2)
        half = 0.5 * v
        inner = half + 0.5 * swapped
        outer = jnp.where(edge_out, 0.0, half + 0.5 * x_other(swapped))
        yp = jnp.where(edge_yp, 0.0, half + 0.5 * roll(v, -1, 2))
        ym = jnp.where(edge_ym, 0.0, half + 0.5 * roll(v, 1, 2))
        m = REACTION + jnp.where(edge_out, half, 0.0) + jnp.where(edge_yp | edge_ym, half, 0.0)
        m = m + jnp.where(before > 0, 0.0, half) + jnp.where(after > 0, 0.0, half)
        cin[pl.ds(p, n)] = inner
        cout[pl.ds(p, n)] = outer
        cyp[pl.ds(p, n)] = yp
        cym[pl.ds(p, n)] = ym
        mass[pl.ds(p, n)] = m
        od[pl.ds(p, n)] = RELAX / (m + inner + outer + yp + ym + cz[pl.ds(p - 1, n)] + cz[pl.ds(p, n)])

    chunked(1, W - 1, C, fine_coeffs)

    def gather_block(fine, n):
        t = fine.reshape(n, 2, sz.rows, sz.lanes)
        t = t[:, 0] + t[:, 1]
        t = t + roll(t, sz.width, 2)
        return t + jnp.where(lane % 2 == 0, roll(t, -1, 2), roll(t, 1, 2))

    def coarse_visc(p, n):
        cv[pl.ds(p, n)] = 0.125 * gather_block(visc[pl.ds(2 * p, 2 * n)], n)

    chunked(0, W // 2, C // 2, coarse_visc)

    def coarse_faces(p, n):
        ccz[pl.ds(p, n)] = faces_z(cv, p, n, 2.0)

    chunked(0, W // 2 - 1, C, coarse_faces)
    cedge_yp, cedge_ym = y >= sz.width - 2, y < 2

    def coarse_coeffs(p, n):
        v = cv[pl.ds(p, n)]
        before, after = cv[pl.ds(p - 1, n)], cv[pl.ds(p + 1, n)]
        twice = 2.0 * v
        xp = jnp.where(sub == sz.rows - 1, 0.0, twice + 2.0 * roll(v, -1, 1))
        yp = jnp.where(cedge_yp, 0.0, twice + 2.0 * roll(v, -2, 2))
        ym = jnp.where(cedge_ym, 0.0, twice + 2.0 * roll(v, 2, 2))
        m = 8.0 * REACTION + jnp.where(sub == 0, twice, 0.0) + jnp.where(sub == sz.rows - 1, twice, 0.0)
        m = m + jnp.where(cedge_yp, twice, 0.0) + jnp.where(cedge_ym, twice, 0.0)
        m = m + jnp.where(before > 0, 0.0, twice) + jnp.where(after > 0, 0.0, twice)
        ccx[pl.ds(p, n)] = xp
        ccyp[pl.ds(p, n)] = yp
        ccym[pl.ds(p, n)] = ym
        cmass[pl.ds(p, n)] = m
        cod[pl.ds(p, n)] = RELAX / (m + xp + roll(xp, 1, 1) + yp + ym + ccz[pl.ds(p - 1, n)] + ccz[pl.ds(p, n)])

    chunked(1, W // 2 - 1, C, coarse_coeffs)

    def fine_apply(ref, p, n):
        ext = ref[pl.ds(p - 1, n + 2)]
        v = ext[1 : n + 1]
        flux = cz[pl.ds(p - 1, n + 1)] * (ext[: n + 1] - ext[1:])
        swapped = roll(v, sz.width, 2)
        out = mass[pl.ds(p, n)] * v + (flux[1:] - flux[:n])
        out = out + cyp[pl.ds(p, n)] * (v - roll(v, -1, 2)) + cym[pl.ds(p, n)] * (v - roll(v, 1, 2))
        return out + cin[pl.ds(p, n)] * (v - swapped) + cout[pl.ds(p, n)] * (v - x_other(swapped))

    def coarse_apply(ref, p, n):
        ext = ref[pl.ds(p - 1, n + 2)]
        v = ext[1 : n + 1]
        flux = ccz[pl.ds(p - 1, n + 1)] * (ext[: n + 1] - ext[1:])
        fx = ccx[pl.ds(p, n)] * (v - roll(v, -1, 1))
        out = cmass[pl.ds(p, n)] * v + (flux[1:] - flux[:n]) + (fx - roll(fx, 1, 1))
        return out + ccyp[pl.ds(p, n)] * (v - roll(v, -2, 2)) + ccym[pl.ds(p, n)] * (v - roll(v, 2, 2))

    def spread(reach, n, body, unit=1):
        chunked((H - reach) // unit, (H + N + reach) // unit, n, body)

    for k in range(ITERS):
        reach = HALO - 1 - k * STEP
        rho, rho_next, u = rhos[k], rhos[k + 1], us[k]

        def smooth(p, n):
            sm[pl.ds(p, n)] = od[pl.ds(p, n)] * rho[pl.ds(p, n)]

        spread(reach, C, smooth)

        def restricted(p, n):
            defect = rho[pl.ds(2 * p, 2 * n)] - fine_apply(sm, 2 * p, 2 * n)
            b = gather_block(defect, n)
            rhs[pl.ds(p, n)] = b
            c0[pl.ds(p, n)] = cod[pl.ds(p, n)] * b

        spread(reach - 1, C // 2, restricted, 2)
        old, new = c0, c1
        for sweep in range(1, CSWEEPS):

            def relax(p, n):
                at = pl.ds(p, n)
                new[at] = old[at] + cod[at] * (rhs[at] - coarse_apply(old, p, n))

            spread(reach - 1 - 2 * sweep, C, relax, 2)
            old, new = new, old
        reach = reach - 1 - 2 * (CSWEEPS - 1)

        def prolonged(p, n):
            c = old[pl.ds(p, n)]
            fine = jnp.stack([c, c], axis=1).reshape(2 * n, sz.rows, sz.lanes)
            sm2[pl.ds(2 * p, 2 * n)] = sm[pl.ds(2 * p, 2 * n)] + fine

        spread(reach, C // 2, prolonged, 2)

        def smoothed(p, n):
            at = pl.ds(p, n)
            u[at] = sm2[at] + od[at] * (rho[at] - fine_apply(sm2, p, n))

        spread(reach - 1, C, smoothed)

        def descend(p, n):
            rho_next[pl.ds(p, n)] = rho[pl.ds(p, n)] - fine_apply(u, p, n)

        spread(reach - 2, C, descend)

    pairs = [(j, k) for j in range(ITERS + 1) for k in range(ITERS)]

    def products(i, sums):
        p = H + i
        rv = [r[p] for r in rhos]
        uv = [u[p] for u in us]
        for k in range(ITERS):
            u_out[k, i] = uv[k]
            rho_out[k, i] = rv[k + 1]
        return tuple(s + rv[j] * uv[k] for s, (j, k) in zip(sums, pairs))

    zero = jnp.zeros((sz.rows, sz.lanes), jnp.float32)
    sums = lax.fori_loop(0, N, products, (zero,) * len(pairs), unroll=4)
    wide = -(-len(pairs) // 8) * 8
    rows = [jnp.sum(s, axis=0, keepdims=True) for s in sums]
    rows = jnp.concatenate(rows + [jnp.zeros((wide - len(rows), sz.lanes), jnp.float32)], axis=0)
    total = jnp.broadcast_to(jnp.sum(rows, axis=1, keepdims=True), rows.shape)
    line = jnp.sum(jnp.where(sub_iota(rows.shape) == lane_iota(rows.shape), total, 0.0), axis=0, keepdims=True)
    gram_out[...] = jnp.broadcast_to(line[None], gram_out.shape)


def combine_kernel(sz, gram_ref, main_ref, u_ref, rho_ref, out_ref, scr):
    line = jnp.sum(gram_ref[...], axis=0)
    lane = lane_iota(line.shape)

    def entry(j, k):
        picked = jnp.where(lane == j * ITERS + k, line, 0.0)
        return jnp.broadcast_to(jnp.sum(picked, axis=1, keepdims=True), line.shape)

    g = [[entry(j, k) for k in range(ITERS)] for j in range(ITERS + 1)]
    zero = jnp.zeros_like(line)
    one = jnp.ones_like(line)

    def form(left, right, matrix):
        total = zero
        for j, a in enumerate(left):
            for k, b in enumerate(right):
                total = total + a * b * matrix(j, k)
        return total

    res = [one]
    direction = [one]
    sol = [zero] * ITERS
    product = g[0][0]
    for i in range(ITERS):
        alpha = product / form(direction, direction, lambda j, k: g[k][j] - g[k + 1][j])
        for k, b in enumerate(direction):
            sol[k] = sol[k] + alpha * b
        res = res + [zero]
        for k, b in enumerate(direction):
            res[k] = res[k] - alpha * b
            res[k + 1] = res[k + 1] + alpha * b
        if i + 1 < ITERS:
            following = form(res, res, lambda j, k: g[j][k])
            beta = following / product
            direction = [a + beta * b for a, b in zip(res, direction + [zero])]
            product = following

    sol = [s.reshape(1, 1, sz.lanes) for s in sol]
    res = [s.reshape(1, 1, sz.lanes) for s in res]

    for a in range(2):

        def body(p, n):
            at = pl.ds(p, n)
            if a == 0:
                v = sum(sol[k] * u_ref[k, at] for k in range(ITERS))
            else:
                v = res[0] * main_ref[0, at] + sum(res[k + 1] * rho_ref[k, at] for k in range(ITERS))
            v = swap_blocks(v, sz.gy, sz.yl)
            rows = pl.multiple_of(p * sz.group, 8)
            scr[pl.ds(rows, n * sz.group), :] = v.reshape(n * sz.group, sz.lanes)

        chunked(0, sz.planes, sz.chunk, body)
        for dest in range(sz.group):
            out_ref[dest, a] = scr[pl.ds(dest, sz.planes, stride=sz.group), :]


def unpack_kernel(sz, in_ref, sol_ref, res_ref):
    for a, out in ((0, sol_ref), (1, res_ref)):
        for c in range(sz.comps):
            halves = [in_ref[part_of(sz, half) * sz.gy + c, a] for half in range(sz.gx)]
            turned = jnp.concatenate(halves, axis=0).T
            for i, x in enumerate(x_order(sz)):
                out[c, x] = turned[i * sz.yl : (i + 1) * sz.yl]


def vmem(count):
    return [pl.BlockSpec(memory_space=pltpu.VMEM)] * count


def call(kernel, sz, ins, outs, scratch=(), name=None):
    outs = [jax.ShapeDtypeStruct(s, jnp.float32) for s in outs]
    held = sum(math.prod(s) for s in [a.shape for a in ins] + [o.shape for o in outs] + list(scratch))
    return pl.pallas_call(
        functools.partial(kernel, sz),
        in_specs=vmem(len(ins)),
        out_specs=vmem(len(outs)),
        out_shape=outs,
        scratch_shapes=[pltpu.VMEM(s, jnp.float32) for s in scratch],
        compiler_params=pltpu.CompilerParams(vmem_limit_bytes=4 * held + 3 * 2**20),
        name=name,
    )(*ins)


def shards(mesh, forcing, viscosity):
    comps, xl, yl, zl = forcing.shape
    sz = Sizes(mesh, comps, xl, yl, zl)
    N, W = sz.planes, sz.window
    plane = (sz.rows, sz.lanes)
    group_shape = (sz.group, 2, N, sz.lanes)
    (packed,) = call(pack_kernel, sz, [forcing, viscosity], [group_shape], name="pack")
    packed = lax.all_to_all(packed, ("gx", "gy"), 0, 0)
    edge_shapes = [(2, c) + plane for c in sz.hops if c < N for _ in range(2)]
    main, *edges = call(
        planes_kernel, sz, [packed], [(2, N) + plane] + edge_shapes, [(N * sz.group, sz.lanes)], name="planes"
    )
    halos = []
    for j, count in enumerate(sz.hops):
        first, last = (edges.pop(0), edges.pop(0)) if count < N else (main, main)
        halos += [to_slab(sz, last, j + 1), to_slab(sz, first, -(j + 1))]
    devices = sz.group * sz.gz
    fine, coarse = (W,) + plane, (W // 2,) + plane
    u, rho, gram = call(
        basis_kernel,
        sz,
        [main] + halos,
        [(ITERS, N) + plane, (ITERS, N) + plane, (devices, 1, sz.lanes)],
        [fine] * 8 + [coarse] * 10 + [fine] * (2 + 2 * ITERS + 1),
        name="basis",
    )
    gram = lax.all_to_all(gram, ("gx", "gy", "gz"), 0, 0)
    (mixed,) = call(
        combine_kernel, sz, [gram, main, u, rho], [group_shape], [(N * sz.group, sz.lanes)], name="combine"
    )
    mixed = lax.all_to_all(mixed, ("gx", "gy"), 0, 0)
    return tuple(call(unpack_kernel, sz, [mixed], [forcing.shape, forcing.shape], name="unpack"))


def solution(mesh):
    spec = P(None, "gx", "gy", "gz")
    return jax.shard_map(
        functools.partial(shards, dict(mesh.shape)),
        mesh=mesh,
        in_specs=(spec, P("gx", "gy", "gz")),
        out_specs=(spec, spec),
        check_vma=False,
    )
```

```python
import functools
import math
import jax
import jax.numpy as jnp
from jax import lax
from jax.experimental import pallas as pl
from jax.experimental.pallas import tpu as pltpu
from jax.sharding import PartitionSpec as P

ITERS = 3
CSWEEPS = 4
REACTION = 1.0
RELAX = 2.0 / 3.0

STEP = 2 * (CSWEEPS - 1) + 4
HALO = ITERS * STEP
BLOCK_ROWS = 1024
STATE_LIMIT = 6 * 2**20


def lane_iota(shape):
    return lax.broadcasted_iota(jnp.int32, shape, len(shape) - 1)


def sub_iota(shape):
    return lax.broadcasted_iota(jnp.int32, shape, len(shape) - 2)


def roll(v, shift, dim):
    size = v.shape[dim]
    return pltpu.roll(v, shift % size, dim)


def swap_blocks(v, count, width):
    sub, lane = sub_iota(v.shape), lane_iota(v.shape)
    step = 1
    while step < count:
        low = (sub // step) % 2 == 1
        high = (lane // (step * width)) % 2 == 1
        rows, lanes = v.ndim - 2, v.ndim - 1
        from_left = roll(roll(v, step, rows), -step * width, lanes)
        from_right = roll(roll(v, -step, rows), step * width, lanes)
        v = jnp.where(low == high, v, jnp.where(low, from_left, from_right))
        step *= 2
    return v


def chunked(lo, hi, n, body):
    n = min(n, hi - lo)
    count = -(-(hi - lo) // n)
    if count == 1:
        body(lo, n)
        return

    @pl.loop(0, count)
    def _(i):
        body(jnp.minimum(lo + i * n, hi - n), n)


class Sizes:
    def __init__(self, mesh, comps, xl, yl, zl):
        self.gx, self.gy, self.gz = (mesh[a] for a in ("gx", "gy", "gz"))
        self.comps, self.xl, self.yl, self.zl = comps, xl, yl, zl
        self.group = self.gx * self.gy
        self.planes = zl // self.gx
        self.rows = self.gx * xl // 2
        self.width = self.gy * yl
        self.lanes = xl * yl
        self.window = self.planes + 2 * HALO
        self.chunk = max(2, BLOCK_ROWS // self.rows)
        self.hops = []
        left = HALO
        while left > 0:
            self.hops.append(min(left, self.planes))
            left -= self.planes
        self.paired = len(self.hops) == 1 and HALO < self.planes
        assert comps <= self.gy and xl == 2 * self.gy
        assert zl % self.gx == 0 and self.planes % 2 == 0 and self.window % 4 == 0 and 2 * self.width == self.lanes


def slab_of(sz, i):
    z, k = divmod(i, sz.gx)
    return (k if z % 2 == 0 else sz.gx - 1 - k) * sz.gz + z


def to_slab(sz, x, moves):
    n = sz.gx * sz.gz
    perm = [(slab_of(sz, i), slab_of(sz, j)) for i, j in moves(n) if 0 <= j < n]
    return lax.ppermute(x, ("gx", "gz"), perm)


def shifted(x, sz, by):
    return to_slab(sz, x, lambda n: [(i, i + by) for i in range(n)])


def swapped_pairs(x, sz, first):
    return to_slab(sz, x, lambda n: [(i, i + 1 if (i - first) % 2 == 0 else i - 1) for i in range(n)])


def odd_slab(sz):
    place = lax.axis_index("gx")
    line = lax.axis_index("gz")
    place = jnp.where(line % 2 == 1, sz.gx - 1 - place, place)
    return (line * sz.gx + place) % 2 == 1


def x_order(sz):
    return list(range(0, sz.xl, 2)) + list(range(1, sz.xl, 2))


def part_of(sz, half):
    odd = lax.axis_index("gz") % 2
    return jnp.where(odd == 1, sz.gx - 1 - half, half)


def pack_kernel(sz, f_hbm, v_hbm, out_ref, f_ref, v_ref, sems):
    copies = [pltpu.make_async_copy(v_hbm, v_ref, sems.at[0])]
    copies += [pltpu.make_async_copy(f_hbm.at[c], f_ref.at[c], sems.at[1 + c]) for c in range(sz.comps)]
    for copy in copies:
        copy.start()

    def turned(at):
        return jnp.concatenate([at(x) for x in x_order(sz)], axis=0).T

    def put(c, a, field):
        for half in range(sz.gx):
            out_ref[part_of(sz, half) * sz.gy + c, a] = field[half * sz.planes : (half + 1) * sz.planes]

    for c in range(sz.comps, sz.gy):
        for a in range(2):
            put(c, a, jnp.zeros((sz.zl, sz.lanes), jnp.float32))
    copies[0].wait()
    visc = turned(lambda x: v_ref[x])
    for c in range(sz.comps):
        put(c, 1, visc)
    for c in range(sz.comps):
        copies[1 + c].wait()
        put(c, 0, turned(lambda x: f_ref[c, x]))


def planes_kernel(sz, in_ref, main_ref, *rest):
    edges, scr = rest[:-1], rest[-1]
    for a in range(2):
        for src in range(sz.group):
            scr[pl.ds(src, sz.planes, stride=sz.group), :] = in_ref[src, a]

        def body(p, n):
            rows = pl.multiple_of(p * sz.group, 8)
            v = scr[pl.ds(rows, n * sz.group), :].reshape(n, sz.group, sz.lanes)
            main_ref[a, pl.ds(p, n)] = swap_blocks(v, sz.gy, sz.yl)

        chunked(0, sz.planes, sz.chunk, body)
        k = 0
        for count in sz.hops:
            if sz.paired:
                lo, hi = 0, sz.planes - count
                odd = odd_slab(sz)
                edges[0][a] = main_ref[a, pl.ds(jnp.where(odd, lo, hi), count)]
                edges[1][a] = main_ref[a, pl.ds(jnp.where(odd, hi, lo), count)]
            elif count < sz.planes:
                edges[k][a] = main_ref[a, 0:count]
                edges[k + 1][a] = main_ref[a, sz.planes - count : sz.planes]
                k += 2


FINE_ARRAYS = 14 + 3 * ITERS + ITERS + 1
COARSE_ARRAYS = 9 + ITERS * CSWEEPS


def basis_kernel(phase, sz, *refs):
    it = iter(refs)
    main_ref = next(it) if phase != 1 else None
    halos = [next(it) for _ in range(2 * len(sz.hops))] if phase != 0 else None
    if phase == 1:
        next(it), next(it)
    if phase == 1 or phase == 0:
        fine_state, coarse_state = next(it), next(it)
    u_out, rho_out, gram_out = (next(it) for _ in range(3)) if phase != 0 else (None,) * 3
    if phase is None:
        fine_state, coarse_state = next(it), next(it)
    it = iter([fine_state.at[i] for i in range(FINE_ARRAYS)])
    half, cin, cout, cyp, cym, cz, mass, od = (next(it) for _ in range(8))
    sin, sout, syp, sym, szp, szm = (next(it) for _ in range(6))
    sms, sm2s, us = ([next(it) for _ in range(ITERS)] for _ in range(3))
    rhos = [next(it) for _ in range(ITERS + 1)]
    it = iter([coarse_state.at[i] for i in range(COARSE_ARRAYS)])
    twice, ccz, cod, kxp, kxm, kyp, kym, kzp, kzm = (next(it) for _ in range(9))
    corrections = [[next(it) for _ in range(CSWEEPS)] for _ in range(ITERS)]

    H, N, W, C = HALO, sz.planes, sz.window, sz.chunk
    Q, QC = W // 2, W // 4

    def run(outer, inner, end, n, body, ref=None):
        cut = min(inner, end)
        lo, hi = {None: (outer, end), 0: (cut, end), 1: (outer, cut)}[phase]
        if lo < hi:
            chunked(lo, hi, n, body)
            if ref is not None and hi == end:
                ref[end] = roll(ref[end - 1], sz.width, ref.ndim - 2)

    plane = (1, sz.rows, sz.lanes)
    lane, sub = lane_iota(plane), sub_iota(plane)
    below = lane < sz.width
    y = lane % sz.width
    last = sub == sz.rows - 1

    def plane_at(a, p):
        if H <= p < H + N:
            return main_ref[a, p - H]
        if sz.paired:
            own, other = (halos[i][a, p if p < H else p - H - N] for i in (0, 1))
            return jnp.where(odd_slab(sz) == (p < H), own, other)
        lo, hi = H, H + N
        for j, count in enumerate(sz.hops):
            if lo - count <= p < lo:
                return halos[2 * j][a, p - lo + count]
            if hi <= p < hi + count:
                return halos[2 * j + 1][a, p - hi]
            lo, hi = lo - count, hi + count

    for a, ref in ((1, half), (0, rhos[0])):

        def place(q, n):
            p = jnp.stack([plane_at(a, q + i) for i in range(n)])
            m = jnp.stack([plane_at(a, W - 1 - q - i) for i in range(n)])
            if a == 1:
                p, m = 0.5 * p, 0.5 * m
            ref[q : q + n, 0] = jnp.where(below, p, roll(m, sz.width, 2))
            ref[q : q + n, 1] = jnp.where(below, roll(p, sz.width, 2), m)

        run(0, H, Q, Q, place, half if a == 1 else None)

    def count_of(*edges):
        return sum(e.astype(jnp.float32) for e in edges)

    def z_faces(cells, faces, inner, size):
        def body(q, n):
            faces[pl.ds(q, n)] = cells[pl.ds(q, n)] + cells[pl.ds(q + 1, n)]

        run(0, inner, size, C // 2, body)

    def close_z(cells, faces, first, step, mass_ref=None):
        if phase == 0:
            return
        for q in range(first, -1, -step):
            outside = ~((cells[q] > 0) & (cells[q + 1] > 0))
            total = faces[q]
            faces[q] = jnp.where(outside, 0.0, total)
            if mass_ref is not None:
                moved = jnp.where(outside, total, 0.0)
                for near in (q, q + 1):
                    if near > 0:
                        mass_ref[near] = mass_ref[near] + moved

    z_faces(half, cz, H, Q)
    edge_out = (sub == 0, last)
    edge_y = y == sz.width - 1

    def fine_coeffs(q, n):
        at, under = pl.ds(q, n), pl.ds(q - 1, n)
        h = [half[at, i] for i in (0, 1)]
        inner = h[0] + h[1]
        outer = [None, jnp.where(last, 0.0, h[1] + roll(h[0], -1, 1))]
        outer[0] = roll(outer[1], 1, 1)
        for i in (0, 1):
            yp = jnp.where(edge_y, 0.0, h[i] + roll(h[i], -1, 2))
            ym = roll(yp, 1, 2)
            m = REACTION + count_of(edge_out[i], edge_y, y == 0) * h[i]
            scale = RELAX / (m + inner + outer[i] + (yp + ym) + (cz[under, i] + cz[at, i]))
            cin[at, i], cout[at, i], cyp[at, i], cym[at, i] = inner, outer[i], yp, ym
            mass[at, i], od[at, i] = m, scale
            sin[at, i], sout[at, i], syp[at, i], sym[at, i] = scale * inner, scale * outer[i], scale * yp, scale * ym

    run(1, H + 1, Q, C // 2, fine_coeffs)
    close_z(half, cz, H - 1, N, mass)

    def fine_z(q, n):
        at = pl.ds(q, n)
        szp[at] = od[at] * cz[at]
        szm[at] = od[at] * cz[pl.ds(q - 1, n)]

    run(1, H + 1, Q, C // 2, fine_z)

    def gather_block(fine, n):
        t = fine.reshape(n, 2, sz.rows, sz.lanes)
        t = t[:, 0] + t[:, 1]
        return t + jnp.where(lane % 2 == 0, roll(t, -1, 2), roll(t, 1, 2))

    def coarse_visc(q, n):
        fine = pl.ds(2 * q, 2 * n)
        twice[pl.ds(q, n)] = 0.5 * gather_block(half[fine, 0] + half[fine, 1], n)

    run(0, H // 2, QC, C // 4, coarse_visc, twice)
    z_faces(twice, ccz, H // 2, QC)
    edge_y2 = y >= sz.width - 2
    outer_coarse = count_of(sub == 0, last, edge_y2, y < 2)

    def coarse_coeffs(q, n):
        at = pl.ds(q, n)
        t = twice[at]
        xp = jnp.where(last, 0.0, t + roll(t, -1, 1))
        yp = jnp.where(edge_y2, 0.0, t + roll(t, -2, 2))
        xm, ym = roll(xp, 1, 1), roll(yp, 2, 2)
        m = 8.0 * REACTION + outer_coarse * t
        scale = RELAX / (m + (xp + xm) + (yp + ym) + (ccz[pl.ds(q - 1, n)] + ccz[at]))
        cod[at] = scale
        kxp[at], kxm[at], kyp[at], kym[at] = scale * xp, scale * xm, scale * yp, scale * ym

    run(1, H // 2 + 1, QC, C // 2, coarse_coeffs)
    close_z(twice, ccz, H // 2 - 1, N // 2)

    def coarse_z(q, n):
        at = pl.ds(q, n)
        kzp[at] = cod[at] * ccz[at]
        kzm[at] = cod[at] * ccz[pl.ds(q - 1, n)]

    run(1, H // 2 + 1, QC, C // 2, coarse_z)

    def fine_beside(ref, q, n, coeffs):
        at, under, over = pl.ds(q, n), pl.ds(q - 1, n), pl.ds(q + 1, n)
        inner, outer, yp, ym, z_over, z_under = coeffs
        out = []
        for i in (0, 1):
            v, w = ref[at, i], ref[at, 1 - i]
            total = inner[at, i] * w + outer[at, i] * roll(w, -1 if i else 1, 1)
            total = total + (z_over(at, under, i) * ref[over, i] + z_under(at, under, i) * ref[under, i])
            out.append(total + (yp[at, i] * roll(v, -1, 2) + ym[at, i] * roll(v, 1, 2)))
        return out

    plain = (cin, cout, cyp, cym, lambda at, under, i: cz[at, i], lambda at, under, i: cz[under, i])
    scaled = (sin, sout, syp, sym, lambda at, under, i: szp[at, i], lambda at, under, i: szm[at, i])

    def fine_apply(ref, q, n):
        at = pl.ds(q, n)
        v = [ref[at, i] for i in (0, 1)]
        fin = cin[at, 0] * (v[0] - v[1])
        fout = cout[at, 1] * (v[1] - roll(v[0], -1, 1))
        fx = (fin - roll(fout, 1, 1), fout - fin)
        out = []
        for i in (0, 1):
            ext = ref[pl.ds(q - 1, n + 2), i]
            flux = cz[pl.ds(q - 1, n + 1), i] * (ext[: n + 1] - ext[1:])
            fy = cyp[at, i] * (v[i] - roll(v[i], -1, 2))
            out.append(mass[at, i] * v[i] + (flux[1:] - flux[:n]) + (fy - roll(fy, 1, 2)) + fx[i])
        return out

    known = H
    for k in range(ITERS):
        outer = H - (HALO - 1 - k * STEP)
        rho, rho_next, u, sm, sm2 = rhos[k], rhos[k + 1], us[k], sms[k], sm2s[k]

        def smooth(q, n):
            sm[pl.ds(q, n)] = od[pl.ds(q, n)] * rho[pl.ds(q, n)]

        known = max(known, H + 1)
        run(outer, known, Q, C // 2, smooth, sm)

        first = corrections[k][0]

        def restricted(q, n):
            fine = pl.ds(2 * q, 2 * n)
            left, right = fine_beside(sm, 2 * q, 2 * n, plain)
            defect = (1.0 - RELAX) * (rho[fine, 0] + rho[fine, 1]) + (left + right)
            first[pl.ds(q, n)] = cod[pl.ds(q, n)] * gather_block(defect, n)

        outer, known = (outer + 1) // 2, (known + 2) // 2
        run(outer, known, QC, C // 4, restricted, first)
        for old, new in zip(corrections[k], corrections[k][1:]):

            def relax(q, n):
                at = pl.ds(q, n)
                v = old[at]
                total = first[at] + (1.0 - RELAX) * v
                total = total + (kzp[at] * old[pl.ds(q + 1, n)] + kzm[at] * old[pl.ds(q - 1, n)])
                total = total + (kxp[at] * roll(v, -1, 1) + kxm[at] * roll(v, 1, 1))
                new[at] = total + (kyp[at] * roll(v, -2, 2) + kym[at] * roll(v, 2, 2))

            outer, known = outer + 1, known + 1
            run(outer, known, QC, C // 2, relax, new)

        def prolonged(q, n):
            c = new[pl.ds(q, n)]
            fine = jnp.stack([c, c], axis=1).reshape(2 * n, sz.rows, sz.lanes)
            for i in (0, 1):
                sm2[pl.ds(2 * q, 2 * n), i] = sm[pl.ds(2 * q, 2 * n), i] + fine

        run(outer, known, QC, C // 4, prolonged)
        if phase is None or phase == (0 if known < QC else 1):
            sm2[Q] = roll(sm2[Q - 1], sz.width, 2)

        def smoothed(q, n):
            at = pl.ds(q, n)
            for i, beside in enumerate(fine_beside(sm2, q, n, scaled)):
                u[at, i] = (1.0 - RELAX) * sm2[at, i] + sm[at, i] + beside

        outer, known = 2 * outer + 1, 2 * known + 1
        run(outer, known, Q, C // 2, smoothed, u)

        def descend(q, n):
            at = pl.ds(q, n)
            for i, image in enumerate(fine_apply(u, q, n)):
                rho_next[at, i] = rho[at, i] - image

        outer, known = outer + 1, known + 1
        run(outer, known, Q, C // 2, descend)

    if phase == 0:
        return
    pairs = [(j, k) for j in range(ITERS + 1) for k in range(ITERS)]

    def products(q, sums):
        for i in (0, 1):
            rv = [r[H + q, i] for r in rhos]
            uv = [u[H + q, i] for u in us]
            for k in range(ITERS):
                u_out[k, q, i] = uv[k]
            for j in range(ITERS + 1):
                rho_out[j, q, i] = rv[j]
            sums = tuple(s + rv[j] * uv[k] for s, (j, k) in zip(sums, pairs))
        return sums

    zero = jnp.zeros((sz.rows, sz.lanes), jnp.float32)
    sums = lax.fori_loop(0, N // 2, products, (zero,) * len(pairs), unroll=4)
    wide = -(-len(pairs) // 8) * 8
    rows = [jnp.sum(s, axis=0, keepdims=True) for s in sums]
    rows = jnp.concatenate(rows + [jnp.zeros((wide - len(rows), sz.lanes), jnp.float32)], axis=0)
    total = jnp.broadcast_to(jnp.sum(rows, axis=1, keepdims=True), rows.shape)
    line = jnp.sum(jnp.where(sub_iota(rows.shape) == lane_iota(rows.shape), total, 0.0), axis=0, keepdims=True)
    gram_out[...] = jnp.broadcast_to(line[None], gram_out.shape)


def combine_kernel(sz, gram_ref, u_ref, rho_ref, out_ref, scr):
    line = jnp.sum(gram_ref[...], axis=0)
    lane = lane_iota(line.shape)

    def entry(j, k):
        picked = jnp.where(lane == j * ITERS + k, line, 0.0)
        return jnp.broadcast_to(jnp.sum(picked, axis=1, keepdims=True), line.shape)

    g = [[entry(j, k) for k in range(ITERS)] for j in range(ITERS + 1)]
    zero = jnp.zeros_like(line)
    one = jnp.ones_like(line)

    def form(left, right, matrix):
        total = zero
        for j, a in enumerate(left):
            for k, b in enumerate(right):
                total = total + a * b * matrix(j, k)
        return total

    res = [one]
    direction = [one]
    sol = [zero] * ITERS
    product = g[0][0]
    for i in range(ITERS):
        alpha = product / form(direction, direction, lambda j, k: g[k][j] - g[k + 1][j])
        for k, b in enumerate(direction):
            sol[k] = sol[k] + alpha * b
        res = res + [zero]
        for k, b in enumerate(direction):
            res[k] = res[k] - alpha * b
            res[k + 1] = res[k + 1] + alpha * b
        if i + 1 < ITERS:
            following = form(res, res, lambda j, k: g[j][k])
            beta = following / product
            direction = [a + beta * b for a, b in zip(res, direction + [zero])]
            product = following

    below = lane_iota((1, sz.rows, sz.lanes)) < sz.width
    for a, (ref, weights) in enumerate(((u_ref, sol), (rho_ref, res))):

        def body(q, n):
            left, right = (sum(w * ref[k, pl.ds(q, n), i] for k, w in enumerate(weights)) for i in (0, 1))
            under = swap_blocks(jnp.where(below, left, roll(right, sz.width, 2)), sz.gy, sz.yl)
            over = swap_blocks(jnp.where(below, roll(left, sz.width, 2), right), sz.gy, sz.yl)
            for i in range(n):
                for p, v in ((q + i, under), (sz.planes - 1 - q - i, over)):
                    row = p * sz.group if isinstance(p, int) else pl.multiple_of(p * sz.group, 8)
                    scr[pl.ds(row, sz.group), :] = v[i]

        chunked(0, sz.planes // 2, sz.chunk // 2, body)
        for dest in range(sz.group):
            out_ref[dest, a] = scr[pl.ds(dest, sz.planes, stride=sz.group), :]


def unpack_kernel(sz, in_ref, sol_ref, res_ref):
    for a, out in ((0, sol_ref), (1, res_ref)):
        for c in range(sz.comps):
            halves = [in_ref[part_of(sz, half) * sz.gy + c, a] for half in range(sz.gx)]
            turned = jnp.concatenate(halves, axis=0).T
            for i, x in enumerate(x_order(sz)):
                out[c, x] = turned[i * sz.yl : (i + 1) * sz.yl]


def call(kernel, sz, ins, outs, scratch=(), name=None, sems=0, alias={}):
    outs = [jax.ShapeDtypeStruct(s, jnp.float32) for s in outs]
    own = [a.shape for i, a in enumerate(ins) if i not in alias]
    held = sum(math.prod(s) for s in own + [o.shape for o in outs] + list(scratch))
    scratch = [pltpu.VMEM(s, jnp.float32) for s in scratch]
    return pl.pallas_call(
        functools.partial(kernel, sz),
        in_specs=[pl.BlockSpec(memory_space=pltpu.HBM if sems else pltpu.VMEM)] * len(ins),
        out_specs=[pl.BlockSpec(memory_space=pltpu.VMEM)] * len(outs),
        out_shape=outs,
        scratch_shapes=scratch + ([pltpu.SemaphoreType.DMA((sems,))] if sems else []),
        compiler_params=pltpu.CompilerParams(vmem_limit_bytes=4 * held + 3 * 2**20),
        input_output_aliases=alias,
        name=name,
    )(*ins)


def shards(mesh, forcing, viscosity):
    comps, xl, yl, zl = forcing.shape
    sz = Sizes(mesh, comps, xl, yl, zl)
    N, W = sz.planes, sz.window
    plane = (sz.rows, sz.lanes)
    group_shape = (sz.group, 2, N, sz.lanes)
    arrays = [pltpu.with_memory_space_constraint(a, pltpu.HBM) for a in (forcing, viscosity)]
    (packed,) = call(
        pack_kernel, sz, arrays, [group_shape], [a.shape for a in arrays], name="pack", sems=1 + sz.comps
    )
    packed = lax.all_to_all(packed, ("gx", "gy"), 0, 0)
    edge_shapes = [(2, c) + plane for c in sz.hops if c < N for _ in range(2)]
    main, *edges = call(
        planes_kernel, sz, [packed], [(2, N) + plane] + edge_shapes, [(N * sz.group, sz.lanes)], name="planes"
    )
    halos = []
    if sz.paired:
        halos = [swapped_pairs(edge, sz, first) for first, edge in reversed(list(enumerate(edges)))][::-1]
    for j, count in enumerate([] if sz.paired else sz.hops):
        first, last = (edges.pop(0), edges.pop(0)) if count < N else (main, main)
        halos += [shifted(last, sz, j + 1), shifted(first, sz, -(j + 1))]
    devices = sz.group * sz.gz
    own = (N // 2, 2) + plane
    state = [(FINE_ARRAYS, W // 2 + 1, 2) + plane, (COARSE_ARRAYS, W // 4 + 1) + plane]
    results = [(ITERS,) + own, (ITERS + 1,) + own, (devices, 1, sz.lanes)]
    if sum(math.prod(shape) for shape in state) <= STATE_LIMIT:
        held = call(functools.partial(basis_kernel, 0), sz, [main], state, name="inner")
        ins = halos + list(held)
        alias = {len(halos): 0, len(halos) + 1: 1}
        *_, u, rho, gram = call(functools.partial(basis_kernel, 1), sz, ins, state + results, name="outer", alias=alias)
    else:
        u, rho, gram = call(functools.partial(basis_kernel, None), sz, [main] + halos, results, state, name="basis")
    gram = lax.all_to_all(gram, ("gx", "gy", "gz"), 0, 0)
    (mixed,) = call(
        combine_kernel, sz, [gram, u, rho], [group_shape], [(N * sz.group, sz.lanes)], name="combine"
    )
    mixed = lax.all_to_all(mixed, ("gx", "gy"), 0, 0)
    return tuple(call(unpack_kernel, sz, [mixed], [forcing.shape, forcing.shape], name="unpack"))


def solution(mesh):
    spec = P(None, "gx", "gy", "gz")
    return jax.shard_map(
        functools.partial(shards, dict(mesh.shape)),
        mesh=mesh,
        in_specs=(spec, P("gx", "gy", "gz")),
        out_specs=(spec, spec),
        check_vma=False,
    )
```

```python
import functools
import math
import jax
import jax.numpy as jnp
from jax import lax
from jax.experimental import pallas as pl
from jax.experimental.pallas import tpu as pltpu
from jax.sharding import PartitionSpec as P

ITERS = 3
CSWEEPS = 4
REACTION = 1.0
RELAX = 2.0 / 3.0

STEP = 2 * (CSWEEPS - 1) + 4
HALO = ITERS * STEP
MOMENTS = 2 * ITERS - 1
BLOCK_ROWS = 1024
GROUP = ("gy", "gx")
STATE_LIMIT = 6 * 2**20


def lane_iota(shape):
    return lax.broadcasted_iota(jnp.int32, shape, len(shape) - 1)


def sub_iota(shape):
    return lax.broadcasted_iota(jnp.int32, shape, len(shape) - 2)


def roll(v, shift, dim):
    size = v.shape[dim]
    return pltpu.roll(v, shift % size, dim)


def swap_blocks(v, count, width):
    sub, lane = sub_iota(v.shape), lane_iota(v.shape)
    step = 1
    while step < count:
        low = (sub // step) % 2 == 1
        high = (lane // (step * width)) % 2 == 1
        rows, lanes = v.ndim - 2, v.ndim - 1
        from_left = roll(roll(v, step, rows), -step * width, lanes)
        from_right = roll(roll(v, -step, rows), step * width, lanes)
        v = jnp.where(low == high, v, jnp.where(low, from_left, from_right))
        step *= 2
    return v


def two_sum(a, b):
    s = a + b
    t = s - a
    return s, (a - (s - t)) + (b - t)


class Pair:
    def __init__(self, hi, lo):
        self.hi, self.lo = hi, lo

    @staticmethod
    def of(hi, lo):
        s = hi + lo
        return Pair(s, lo - (s - hi))

    def __add__(self, other):
        s, e = two_sum(self.hi, other.hi)
        return Pair.of(s, e + (self.lo + other.lo))

    def __neg__(self):
        return Pair(-self.hi, -self.lo)

    def __sub__(self, other):
        return self + -other

    def twice(self):
        return Pair(2.0 * self.hi, 2.0 * self.lo)

    def __mul__(self, other):
        p = self.hi * other.hi
        (a, b), (c, d) = split(self.hi), split(other.hi)
        e = ((a * c - p) + a * d + b * c) + b * d
        return Pair.of(p, e + (self.hi * other.lo + self.lo * other.hi))

    def __truediv__(self, other):
        q = self.hi / other.hi
        rest = self - other * Pair(q, jnp.zeros_like(q))
        return Pair.of(q, rest.hi / other.hi)


def split(a):
    t = 4097.0 * a
    hi = t - (t - a)
    return hi, a - hi


def total(terms):
    return functools.reduce(lambda a, b: a + b, terms)


def chunked(lo, hi, n, body):
    n = min(n, hi - lo)
    count = -(-(hi - lo) // n)
    if count == 1:
        body(lo, n)
        return

    @pl.loop(0, count)
    def _(i):
        body(jnp.minimum(lo + i * n, hi - n), n)


class Sizes:
    def __init__(self, mesh, comps, xl, yl, zl):
        self.gx, self.gy, self.gz = (mesh[a] for a in ("gx", "gy", "gz"))
        self.comps, self.xl, self.yl, self.zl = comps, xl, yl, zl
        self.group = self.gx * self.gy
        self.planes = zl // self.gx
        self.rows = self.gx * xl // 2
        self.width = self.gy * yl
        self.lanes = xl * yl
        self.window = self.planes + 2 * HALO
        self.chunk = max(2, BLOCK_ROWS // self.rows)
        self.hops = []
        left = HALO
        while left > 0:
            self.hops.append(min(left, self.planes))
            left -= self.planes
        self.paired = len(self.hops) == 1 and HALO < self.planes
        assert comps <= self.gy and xl == 2 * self.gy
        assert zl % self.gx == 0 and self.planes % 2 == 0 and self.window % 4 == 0 and 2 * self.width == self.lanes


def slab_of(sz, i):
    z, k = divmod(i, sz.gx)
    return (k if z % 2 == 0 else sz.gx - 1 - k) * sz.gz + z


def to_slab(sz, x, moves):
    n = sz.gx * sz.gz
    perm = [(slab_of(sz, i), slab_of(sz, j)) for i, j in moves(n) if 0 <= j < n]
    return lax.ppermute(x, ("gx", "gz"), perm)


def shifted(x, sz, by):
    return to_slab(sz, x, lambda n: [(i, i + by) for i in range(n)])


def swapped_pairs(x, sz, first):
    return to_slab(sz, x, lambda n: [(i, i + 1 if (i - first) % 2 == 0 else i - 1) for i in range(n)])


def odd_slab(sz):
    place = lax.axis_index("gx")
    line = lax.axis_index("gz")
    place = jnp.where(line % 2 == 1, sz.gx - 1 - place, place)
    return (line * sz.gx + place) % 2 == 1


def x_order(sz):
    return list(range(0, sz.xl, 2)) + list(range(1, sz.xl, 2))


def member_of(sz, x, y):
    return y * sz.gx + x if GROUP[0] == "gy" else x * sz.gy + y


def row_of(sz, member):
    return member % sz.gx * sz.gy + member // sz.gx if GROUP[0] == "gy" else member


def part_of(sz, half):
    odd = lax.axis_index("gz") % 2
    return jnp.where(odd == 1, sz.gx - 1 - half, half)


def pack_kernel(sz, f_hbm, v_hbm, out_ref, f_ref, v_ref, sems):
    copies = [pltpu.make_async_copy(v_hbm, v_ref, sems.at[0])]
    copies += [pltpu.make_async_copy(f_hbm.at[c], f_ref.at[c], sems.at[1 + c]) for c in range(sz.comps)]
    for copy in copies:
        copy.start()

    def turned(at):
        return jnp.concatenate([at(x) for x in x_order(sz)], axis=0).T

    def put(c, a, field):
        for half in range(sz.gx):
            out_ref[member_of(sz, part_of(sz, half), c), a] = field[half * sz.planes : (half + 1) * sz.planes]

    for c in range(sz.comps, sz.gy):
        for a in range(2):
            put(c, a, jnp.zeros((sz.zl, sz.lanes), jnp.float32))
    copies[0].wait()
    visc = turned(lambda x: v_ref[x])
    for c in range(sz.comps):
        put(c, 1, visc)
    for c in range(sz.comps):
        copies[1 + c].wait()
        put(c, 0, turned(lambda x: f_ref[c, x]))


def planes_kernel(sz, in_ref, main_ref, *rest):
    edges, scr = rest[:-1], rest[-1]
    for a in range(2):
        for src in range(sz.group):
            scr[pl.ds(row_of(sz, src), sz.planes, stride=sz.group), :] = in_ref[src, a]

        def body(p, n):
            rows = pl.multiple_of(p * sz.group, 8)
            v = scr[pl.ds(rows, n * sz.group), :].reshape(n, sz.group, sz.lanes)
            main_ref[a, pl.ds(p, n)] = swap_blocks(v, sz.gy, sz.yl)

        chunked(0, sz.planes, sz.chunk, body)
        k = 0
        for count in sz.hops:
            if sz.paired:
                lo, hi = 0, sz.planes - count
                odd = odd_slab(sz)
                edges[0][a] = main_ref[a, pl.ds(jnp.where(odd, lo, hi), count)]
                edges[1][a] = main_ref[a, pl.ds(jnp.where(odd, hi, lo), count)]
            elif count < sz.planes:
                edges[k][a] = main_ref[a, 0:count]
                edges[k + 1][a] = main_ref[a, sz.planes - count : sz.planes]
                k += 2


FINE_ARRAYS = 14 + 3 * ITERS + ITERS + 1
COARSE_ARRAYS = 9 + ITERS * CSWEEPS


def basis_kernel(phase, sz, *refs):
    it = iter(refs)
    main_ref = next(it) if phase != 1 else None
    halos = [next(it) for _ in range(2 * len(sz.hops))] if phase != 0 else None
    if phase == 1:
        next(it), next(it)
    if phase == 1 or phase == 0:
        fine_state, coarse_state = next(it), next(it)
    if phase is None:
        fine_state, coarse_state = next(it), next(it)
    gram_out = next(it) if phase != 0 else None
    it = iter([fine_state.at[i] for i in range(FINE_ARRAYS)])
    us = [next(it) for _ in range(ITERS)]
    rhos = [next(it) for _ in range(ITERS + 1)]
    half, cin, cout, cyp, cym, cz, mass, od = (next(it) for _ in range(8))
    sin, sout, syp, sym, szp, szm = (next(it) for _ in range(6))
    sms, sm2s = ([next(it) for _ in range(ITERS)] for _ in range(2))
    it = iter([coarse_state.at[i] for i in range(COARSE_ARRAYS)])
    twice, ccz, cod, kxp, kxm, kyp, kym, kzp, kzm = (next(it) for _ in range(9))
    corrections = [[next(it) for _ in range(CSWEEPS)] for _ in range(ITERS)]

    H, N, W, C = HALO, sz.planes, sz.window, sz.chunk
    Q, QC = W // 2, W // 4

    def run(outer, inner, end, n, body, ref=None):
        cut = min(inner, end)
        lo, hi = {None: (outer, end), 0: (cut, end), 1: (outer, cut)}[phase]
        if lo < hi:
            chunked(lo, hi, n, body)
            if ref is not None and hi == end:
                ref[end] = roll(ref[end - 1], sz.width, ref.ndim - 2)

    plane = (1, sz.rows, sz.lanes)
    lane, sub = lane_iota(plane), sub_iota(plane)
    below = lane < sz.width
    y = lane % sz.width
    last = sub == sz.rows - 1

    def plane_at(a, p):
        if H <= p < H + N:
            return main_ref[a, p - H]
        if sz.paired:
            own, other = (halos[i][a, p if p < H else p - H - N] for i in (0, 1))
            return jnp.where(odd_slab(sz) == (p < H), own, other)
        lo, hi = H, H + N
        for j, count in enumerate(sz.hops):
            if lo - count <= p < lo:
                return halos[2 * j][a, p - lo + count]
            if hi <= p < hi + count:
                return halos[2 * j + 1][a, p - hi]
            lo, hi = lo - count, hi + count

    for a, ref in ((1, half), (0, rhos[0])):

        def place(q, n):
            p = jnp.stack([plane_at(a, q + i) for i in range(n)])
            m = jnp.stack([plane_at(a, W - 1 - q - i) for i in range(n)])
            if a == 1:
                p, m = 0.5 * p, 0.5 * m
            ref[q : q + n, 0] = jnp.where(below, p, roll(m, sz.width, 2))
            ref[q : q + n, 1] = jnp.where(below, roll(p, sz.width, 2), m)

        run(0, H, Q, Q, place, half if a == 1 else None)

    def count_of(*edges):
        return sum(e.astype(jnp.float32) for e in edges)

    def z_faces(cells, faces, inner, size):
        def body(q, n):
            faces[pl.ds(q, n)] = cells[pl.ds(q, n)] + cells[pl.ds(q + 1, n)]

        run(0, inner, size, C // 2, body)

    def close_z(cells, faces, first, step, mass_ref=None):
        if phase == 0:
            return
        for q in range(first, -1, -step):
            outside = ~((cells[q] > 0) & (cells[q + 1] > 0))
            total = faces[q]
            faces[q] = jnp.where(outside, 0.0, total)
            if mass_ref is not None:
                moved = jnp.where(outside, total, 0.0)
                for near in (q, q + 1):
                    if near > 0:
                        mass_ref[near] = mass_ref[near] + moved

    z_faces(half, cz, H, Q)
    edge_out = (sub == 0, last)
    edge_y = y == sz.width - 1

    def fine_coeffs(q, n):
        at, under = pl.ds(q, n), pl.ds(q - 1, n)
        h = [half[at, i] for i in (0, 1)]
        inner = h[0] + h[1]
        outer = [None, jnp.where(last, 0.0, h[1] + roll(h[0], -1, 1))]
        outer[0] = roll(outer[1], 1, 1)
        for i in (0, 1):
            yp = jnp.where(edge_y, 0.0, h[i] + roll(h[i], -1, 2))
            ym = roll(yp, 1, 2)
            m = REACTION + count_of(edge_out[i], edge_y, y == 0) * h[i]
            scale = RELAX / (m + inner + outer[i] + (yp + ym) + (cz[under, i] + cz[at, i]))
            cin[at, i], cout[at, i], cyp[at, i], cym[at, i] = inner, outer[i], yp, ym
            mass[at, i], od[at, i] = m, scale
            sin[at, i], sout[at, i], syp[at, i], sym[at, i] = scale * inner, scale * outer[i], scale * yp, scale * ym

    run(1, H + 1, Q, C // 2, fine_coeffs)
    close_z(half, cz, H - 1, N, mass)

    def fine_z(q, n):
        at = pl.ds(q, n)
        szp[at] = od[at] * cz[at]
        szm[at] = od[at] * cz[pl.ds(q - 1, n)]

    run(1, H + 1, Q, C // 2, fine_z)

    def gather_block(fine, n):
        t = fine.reshape(n, 2, sz.rows, sz.lanes)
        t = t[:, 0] + t[:, 1]
        return t + jnp.where(lane % 2 == 0, roll(t, -1, 2), roll(t, 1, 2))

    def coarse_visc(q, n):
        fine = pl.ds(2 * q, 2 * n)
        twice[pl.ds(q, n)] = 0.5 * gather_block(half[fine, 0] + half[fine, 1], n)

    run(0, H // 2, QC, C // 4, coarse_visc, twice)
    z_faces(twice, ccz, H // 2, QC)
    edge_y2 = y >= sz.width - 2
    outer_coarse = count_of(sub == 0, last, edge_y2, y < 2)

    def coarse_coeffs(q, n):
        at = pl.ds(q, n)
        t = twice[at]
        xp = jnp.where(last, 0.0, t + roll(t, -1, 1))
        yp = jnp.where(edge_y2, 0.0, t + roll(t, -2, 2))
        xm, ym = roll(xp, 1, 1), roll(yp, 2, 2)
        m = 8.0 * REACTION + outer_coarse * t
        scale = RELAX / (m + (xp + xm) + (yp + ym) + (ccz[pl.ds(q - 1, n)] + ccz[at]))
        cod[at] = scale
        kxp[at], kxm[at], kyp[at], kym[at] = scale * xp, scale * xm, scale * yp, scale * ym

    run(1, H // 2 + 1, QC, C // 2, coarse_coeffs)
    close_z(twice, ccz, H // 2 - 1, N // 2)

    def coarse_z(q, n):
        at = pl.ds(q, n)
        kzp[at] = cod[at] * ccz[at]
        kzm[at] = cod[at] * ccz[pl.ds(q - 1, n)]

    run(1, H // 2 + 1, QC, C // 2, coarse_z)

    def fine_beside(ref, q, n, coeffs):
        at, under, over = pl.ds(q, n), pl.ds(q - 1, n), pl.ds(q + 1, n)
        inner, outer, yp, ym, z_over, z_under = coeffs
        out = []
        for i in (0, 1):
            v, w = ref[at, i], ref[at, 1 - i]
            total = inner[at, i] * w + outer[at, i] * roll(w, -1 if i else 1, 1)
            total = total + (z_over(at, under, i) * ref[over, i] + z_under(at, under, i) * ref[under, i])
            out.append(total + (yp[at, i] * roll(v, -1, 2) + ym[at, i] * roll(v, 1, 2)))
        return out

    plain = (cin, cout, cyp, cym, lambda at, under, i: cz[at, i], lambda at, under, i: cz[under, i])
    scaled = (sin, sout, syp, sym, lambda at, under, i: szp[at, i], lambda at, under, i: szm[at, i])

    def fine_apply(ref, q, n):
        at = pl.ds(q, n)
        v = [ref[at, i] for i in (0, 1)]
        fin = cin[at, 0] * (v[0] - v[1])
        fout = cout[at, 1] * (v[1] - roll(v[0], -1, 1))
        fx = (fin - roll(fout, 1, 1), fout - fin)
        out = []
        for i in (0, 1):
            ext = ref[pl.ds(q - 1, n + 2), i]
            flux = cz[pl.ds(q - 1, n + 1), i] * (ext[: n + 1] - ext[1:])
            fy = cyp[at, i] * (v[i] - roll(v[i], -1, 2))
            out.append(mass[at, i] * v[i] + (flux[1:] - flux[:n]) + (fy - roll(fy, 1, 2)) + fx[i])
        return out

    known = H
    for k in range(ITERS):
        outer = H - (HALO - 1 - k * STEP)
        rho, rho_next, u, sm, sm2 = rhos[k], rhos[k + 1], us[k], sms[k], sm2s[k]

        def smooth(q, n):
            sm[pl.ds(q, n)] = od[pl.ds(q, n)] * rho[pl.ds(q, n)]

        known = max(known, H + 1)
        run(outer, known, Q, C // 2, smooth, sm)

        first = corrections[k][0]

        def restricted(q, n):
            fine = pl.ds(2 * q, 2 * n)
            left, right = fine_beside(sm, 2 * q, 2 * n, plain)
            defect = (1.0 - RELAX) * (rho[fine, 0] + rho[fine, 1]) + (left + right)
            first[pl.ds(q, n)] = cod[pl.ds(q, n)] * gather_block(defect, n)

        outer, known = (outer + 1) // 2, (known + 2) // 2
        run(outer, known, QC, C // 4, restricted, first)
        for old, new in zip(corrections[k], corrections[k][1:]):

            def relax(q, n):
                at = pl.ds(q, n)
                v = old[at]
                total = first[at] + (1.0 - RELAX) * v
                total = total + (kzp[at] * old[pl.ds(q + 1, n)] + kzm[at] * old[pl.ds(q - 1, n)])
                total = total + (kxp[at] * roll(v, -1, 1) + kxm[at] * roll(v, 1, 1))
                new[at] = total + (kyp[at] * roll(v, -2, 2) + kym[at] * roll(v, 2, 2))

            outer, known = outer + 1, known + 1
            run(outer, known, QC, C // 2, relax, new)

        def prolonged(q, n):
            c = new[pl.ds(q, n)]
            fine = jnp.stack([c, c], axis=1).reshape(2 * n, sz.rows, sz.lanes)
            for i in (0, 1):
                sm2[pl.ds(2 * q, 2 * n), i] = sm[pl.ds(2 * q, 2 * n), i] + fine

        run(outer, known, QC, C // 4, prolonged)
        if phase is None or phase == (0 if known < QC else 1):
            sm2[Q] = roll(sm2[Q - 1], sz.width, 2)

        def smoothed(q, n):
            at = pl.ds(q, n)
            for i, beside in enumerate(fine_beside(sm2, q, n, scaled)):
                u[at, i] = (1.0 - RELAX) * sm2[at, i] + sm[at, i] + beside

        outer, known = 2 * outer + 1, 2 * known + 1
        run(outer, known, Q, C // 2, smoothed, u)

        def descend(q, n):
            at = pl.ds(q, n)
            for i, image in enumerate(fine_apply(u, q, n)):
                rho_next[at, i] = rho[at, i] - image
                image_of[at, i] = image

        image_of = sm2
        outer, known = outer + 1, known + 1
        run(outer, known, Q, C // 2, descend)

    if phase == 0:
        return
    orders = [((n + 1) // 2, n // 2) for n in range(MOMENTS)]
    zero = jnp.zeros((sz.rows, sz.lanes), jnp.float32)
    sums = [(zero, zero)] * (2 * MOMENTS)
    for q in range(H, Q):
        rv, yv, uv = ([[ref[q, i] for i in (0, 1)] for ref in refs] for refs in (rhos[:ITERS], sm2s, us))
        for place, left in enumerate((rv, yv)):
            for n, (j, k) in enumerate(orders):
                hi, lo = sums[place * MOMENTS + n]
                hi, error = two_sum(hi, left[j][0] * uv[k][0] + left[j][1] * uv[k][1])
                sums[place * MOMENTS + n] = (hi, lo + error)
    wide = -(-len(sums) // 8) * 8

    def rows_of(values, fold):
        rows = [fold(v, axis=0, keepdims=True) for v in values]
        return jnp.concatenate(rows + [jnp.zeros((wide - len(rows), sz.lanes), jnp.float32)], axis=0)

    most = jnp.max(rows_of([jnp.abs(hi) for hi, _ in sums], jnp.max), axis=1, keepdims=True)
    grid = float(sz.rows * sz.lanes) * jnp.broadcast_to(most, (wide, sz.lanes))
    coarse = [(hi + grid[n : n + 1]) - grid[n : n + 1] for n, (hi, _) in enumerate(sums)]
    rest = [(hi - c) + lo for c, (hi, lo) in zip(coarse, sums)]
    line = jnp.zeros((1, sz.lanes), jnp.float32)
    for offset, values in ((0, coarse), (wide, rest)):
        rows = rows_of(values, jnp.sum)
        each = jnp.broadcast_to(jnp.sum(rows, axis=1, keepdims=True), rows.shape)
        here = sub_iota(rows.shape) + offset == lane_iota(rows.shape)
        line = line + jnp.sum(jnp.where(here, each, 0.0), axis=0, keepdims=True)
    gram_out[...] = jnp.broadcast_to(line[None], gram_out.shape)


def combine_kernel(sz, gram_ref, fine_ref, out_ref, scr):
    parts = gram_ref[:, 0, :]
    wide = -(-2 * MOMENTS // 8) * 8
    hi, lo = parts, roll(parts, -wide, 1)
    while hi.shape[0] % 16 == 0:
        n = hi.shape[0] // 2
        hi, error = two_sum(hi[:n], hi[n:])
        lo = lo[:n] + lo[n:] + error
    sum_hi, sum_lo = hi[:1], lo[:1]
    for i in range(1, hi.shape[0]):
        sum_hi, error = two_sum(sum_hi, hi[i : i + 1])
        sum_lo = sum_lo + (lo[i : i + 1] + error)
    lane = lane_iota(sum_hi.shape)

    def entry(n):
        halves = []
        for v in (sum_hi, sum_lo):
            picked = jnp.sum(jnp.where(lane == n, v, 0.0), axis=1, keepdims=True)
            halves.append(jnp.broadcast_to(picked, v.shape))
        return Pair.of(*halves)

    moments = [entry(n) for n in range(2 * MOMENTS)]

    def form(v, moments):
        terms = []
        for n in range(2 * len(v) - 1):
            pairs = [(j, n - j) for j in range(len(v)) if j <= n - j < len(v)]
            weight = total([v[j] * v[k] if j == k else (v[j] * v[k]).twice() for j, k in pairs])
            terms.append(weight * moments[n])
        return total(terms)

    zero = Pair(jnp.zeros_like(sum_hi), jnp.zeros_like(sum_hi))
    one = Pair(jnp.ones_like(sum_hi), jnp.zeros_like(sum_hi))
    res, direction, sol = [one], [one], []
    product = moments[0]
    for i in range(ITERS):
        image = form(direction, moments[MOMENTS:]) if i else moments[MOMENTS]
        alpha = product / image
        steps = [alpha * b for b in direction] if i else [alpha]
        sol = [s + t for s, t in zip(sol, steps)] + steps[-1:]
        res = [r - t for r, t in zip(res, steps)] + [zero]
        res = res[:1] + [r + t for r, t in zip(res[1:-1], steps)] + steps[-1:]
        if i + 1 < ITERS:
            following = form(res, moments)
            beta = following / product
            direction = [a + beta * b for a, b in zip(res, direction)] + res[-1:]
            product = following

    sol = [s.hi.reshape(1, 1, sz.lanes) for s in sol]
    res = [s.hi.reshape(1, 1, sz.lanes) for s in res]
    below = lane_iota((1, sz.rows, sz.lanes)) < sz.width
    for a, (first, weights) in enumerate(((0, sol), (ITERS, res))):

        def body(q, n):
            left, right = (
                sum(w * fine_ref[first + k, pl.ds(HALO + q, n), i] for k, w in enumerate(weights)) for i in (0, 1)
            )
            under = swap_blocks(jnp.where(below, left, roll(right, sz.width, 2)), sz.gy, sz.yl)
            over = swap_blocks(jnp.where(below, roll(left, sz.width, 2), right), sz.gy, sz.yl)
            for i in range(n):
                for p, v in ((q + i, under), (sz.planes - 1 - q - i, over)):
                    row = p * sz.group if isinstance(p, int) else pl.multiple_of(p * sz.group, 8)
                    scr[pl.ds(row, sz.group), :] = v[i]

        chunked(0, sz.planes // 2, sz.chunk // 2, body)
        for dest in range(sz.group):
            out_ref[dest, a] = scr[pl.ds(row_of(sz, dest), sz.planes, stride=sz.group), :]


def unpack_kernel(sz, in_ref, sol_ref, res_ref):
    for a, out in ((0, sol_ref), (1, res_ref)):
        for c in range(sz.comps):
            halves = [in_ref[member_of(sz, part_of(sz, half), c), a] for half in range(sz.gx)]
            turned = jnp.concatenate(halves, axis=0).T
            for i, x in enumerate(x_order(sz)):
                out[c, x] = turned[i * sz.yl : (i + 1) * sz.yl]


def call(kernel, sz, ins, outs, scratch=(), name=None, sems=0, alias={}):
    outs = [jax.ShapeDtypeStruct(s, jnp.float32) for s in outs]
    own = [a.shape for i, a in enumerate(ins) if i not in alias]
    held = sum(math.prod(s) for s in own + [o.shape for o in outs] + list(scratch))
    scratch = [pltpu.VMEM(s, jnp.float32) for s in scratch]
    return pl.pallas_call(
        functools.partial(kernel, sz),
        in_specs=[pl.BlockSpec(memory_space=pltpu.HBM if sems else pltpu.VMEM)] * len(ins),
        out_specs=[pl.BlockSpec(memory_space=pltpu.VMEM)] * len(outs),
        out_shape=outs,
        scratch_shapes=scratch + ([pltpu.SemaphoreType.DMA((sems,))] if sems else []),
        compiler_params=pltpu.CompilerParams(vmem_limit_bytes=4 * held + 3 * 2**20),
        input_output_aliases=alias,
        name=name,
    )(*ins)


def shards(mesh, forcing, viscosity):
    comps, xl, yl, zl = forcing.shape
    sz = Sizes(mesh, comps, xl, yl, zl)
    N, W = sz.planes, sz.window
    plane = (sz.rows, sz.lanes)
    group_shape = (sz.group, 2, N, sz.lanes)
    arrays = [pltpu.with_memory_space_constraint(a, pltpu.HBM) for a in (forcing, viscosity)]
    (packed,) = call(
        pack_kernel, sz, arrays, [group_shape], [a.shape for a in arrays], name="pack", sems=1 + sz.comps
    )
    packed = lax.all_to_all(packed, GROUP, 0, 0)
    edge_shapes = [(2, c) + plane for c in sz.hops if c < N for _ in range(2)]
    main, *edges = call(
        planes_kernel, sz, [packed], [(2, N) + plane] + edge_shapes, [(N * sz.group, sz.lanes)], name="planes"
    )
    halos = []
    if sz.paired:
        halos = [swapped_pairs(edge, sz, first) for first, edge in reversed(list(enumerate(edges)))][::-1]
    for j, count in enumerate([] if sz.paired else sz.hops):
        first, last = (edges.pop(0), edges.pop(0)) if count < N else (main, main)
        halos += [shifted(last, sz, j + 1), shifted(first, sz, -(j + 1))]
    devices = sz.group * sz.gz
    state = [(FINE_ARRAYS, W // 2 + 1, 2) + plane, (COARSE_ARRAYS, W // 4 + 1) + plane]
    gram_shape = (devices, 1, sz.lanes)
    if sum(math.prod(shape) for shape in state) <= STATE_LIMIT:
        held = call(functools.partial(basis_kernel, 0), sz, [main], state, name="inner")
        alias = {len(halos): 0, len(halos) + 1: 1}
        outer = functools.partial(basis_kernel, 1)
        fine, _, gram = call(outer, sz, halos + list(held), state + [gram_shape], name="outer", alias=alias)
    else:
        whole = functools.partial(basis_kernel, None)
        fine, _, gram = call(whole, sz, [main] + halos, state + [gram_shape], name="basis")
    gram = lax.all_to_all(gram, ("gx", "gy", "gz"), 0, 0)
    (mixed,) = call(
        combine_kernel, sz, [gram, fine], [group_shape], [(N * sz.group, sz.lanes)], name="combine"
    )
    mixed = lax.all_to_all(mixed, GROUP, 0, 0)
    return tuple(call(unpack_kernel, sz, [mixed], [forcing.shape, forcing.shape], name="unpack"))


def solution(mesh):
    spec = P(None, "gx", "gy", "gz")
    return jax.shard_map(
        functools.partial(shards, dict(mesh.shape)),
        mesh=mesh,
        in_specs=(spec, P("gx", "gy", "gz")),
        out_specs=(spec, spec),
        check_vma=False,
    )
```

```python
import functools
import math
import jax
import jax.numpy as jnp
from jax import lax
from jax.experimental import pallas as pl
from jax.experimental.pallas import tpu as pltpu
from jax.sharding import PartitionSpec as P

ITERS = 3
CSWEEPS = 4
REACTION = 1.0
RELAX = 2.0 / 3.0

STEP = 2 * (CSWEEPS - 1) + 4
HALO = ITERS * STEP
MOMENTS = 2 * ITERS - 1
BLOCK_ROWS = 1024
GROUP = ("gy", "gx")
STATE_LIMIT = 6 * 2**20


def lane_iota(shape):
    return lax.broadcasted_iota(jnp.int32, shape, len(shape) - 1)


def sub_iota(shape):
    return lax.broadcasted_iota(jnp.int32, shape, len(shape) - 2)


def roll(v, shift, dim):
    size = v.shape[dim]
    return pltpu.roll(v, shift % size, dim)


def lane_xor(v, bit):
    flat = v.reshape(-1, v.shape[-1])
    return jnp.take_along_axis(flat, lane_iota(flat.shape) ^ bit, axis=1, mode="promise_in_bounds").reshape(v.shape)


def swap_blocks(v, count, width):
    sub, lane = sub_iota(v.shape), lane_iota(v.shape)
    step = 1
    while step < count:
        low = (sub // step) % 2 == 1
        high = (lane // (step * width)) % 2 == 1
        rows = v.ndim - 2
        moved = lane_xor(v, step * width)
        v = jnp.where(low == high, v, jnp.where(low, roll(moved, step, rows), roll(moved, -step, rows)))
        step *= 2
    return v


def two_sum(a, b):
    s = a + b
    t = s - a
    return s, (a - (s - t)) + (b - t)


class Pair:
    def __init__(self, hi, lo):
        self.hi, self.lo = hi, lo

    @staticmethod
    def of(hi, lo):
        s = hi + lo
        return Pair(s, lo - (s - hi))

    def __add__(self, other):
        s, e = two_sum(self.hi, other.hi)
        return Pair.of(s, e + (self.lo + other.lo))

    def __neg__(self):
        return Pair(-self.hi, -self.lo)

    def __sub__(self, other):
        return self + -other

    def twice(self):
        return Pair(2.0 * self.hi, 2.0 * self.lo)

    def __mul__(self, other):
        p = self.hi * other.hi
        (a, b), (c, d) = split(self.hi), split(other.hi)
        e = ((a * c - p) + a * d + b * c) + b * d
        return Pair.of(p, e + (self.hi * other.lo + self.lo * other.hi))

    def __truediv__(self, other):
        q = self.hi / other.hi
        rest = self - other * Pair(q, jnp.zeros_like(q))
        return Pair.of(q, rest.hi / other.hi)


def split(a):
    t = 4097.0 * a
    hi = t - (t - a)
    return hi, a - hi


def total(terms):
    return functools.reduce(lambda a, b: a + b, terms)


def chunked(lo, hi, n, body):
    n = min(n, hi - lo)
    count = -(-(hi - lo) // n)
    if count == 1:
        body(lo, n)
        return

    @pl.loop(0, count)
    def _(i):
        body(jnp.minimum(lo + i * n, hi - n), n)


class Sizes:
    def __init__(self, mesh, comps, xl, yl, zl):
        self.gx, self.gy, self.gz = (mesh[a] for a in ("gx", "gy", "gz"))
        self.comps, self.xl, self.yl, self.zl = comps, xl, yl, zl
        self.group = self.gx * self.gy
        self.planes = zl // self.gx
        self.rows = self.gx * xl // 2
        self.width = self.gy * yl
        self.lanes = xl * yl
        self.window = self.planes + 2 * HALO
        self.chunk = max(2, BLOCK_ROWS // self.rows)
        self.hops = []
        left = HALO
        while left > 0:
            self.hops.append(min(left, self.planes))
            left -= self.planes
        self.paired = len(self.hops) == 1 and HALO < self.planes
        assert comps <= self.gy and xl == 2 * self.gy
        assert zl % self.gx == 0 and self.planes % 2 == 0 and self.window % 4 == 0 and 2 * self.width == self.lanes


def slab_of(sz, i):
    z, k = divmod(i, sz.gx)
    return (k if z % 2 == 0 else sz.gx - 1 - k) * sz.gz + z


def to_slab(sz, x, moves):
    n = sz.gx * sz.gz
    perm = [(slab_of(sz, i), slab_of(sz, j)) for i, j in moves(n) if 0 <= j < n]
    return lax.ppermute(x, ("gx", "gz"), perm)


def shifted(x, sz, by):
    return to_slab(sz, x, lambda n: [(i, i + by) for i in range(n)])


def swapped_pairs(x, sz, first):
    return to_slab(sz, x, lambda n: [(i, i + 1 if (i - first) % 2 == 0 else i - 1) for i in range(n)])


def odd_slab(sz):
    place = lax.axis_index("gx")
    line = lax.axis_index("gz")
    place = jnp.where(line % 2 == 1, sz.gx - 1 - place, place)
    return (line * sz.gx + place) % 2 == 1


def x_order(sz):
    return list(range(0, sz.xl, 2)) + list(range(1, sz.xl, 2))


def member_of(sz, x, y):
    return y * sz.gx + x if GROUP[0] == "gy" else x * sz.gy + y


def row_of(sz, member):
    return member % sz.gx * sz.gy + member // sz.gx if GROUP[0] == "gy" else member


def part_of(sz, half):
    odd = lax.axis_index("gz") % 2
    return jnp.where(odd == 1, sz.gx - 1 - half, half)


def pack_kernel(sz, f_hbm, v_hbm, out_ref, f_ref, v_ref, sems):
    copies = [pltpu.make_async_copy(v_hbm, v_ref, sems.at[0])]
    copies += [pltpu.make_async_copy(f_hbm.at[c], f_ref.at[c], sems.at[1 + c]) for c in range(sz.comps)]
    for copy in copies:
        copy.start()

    def turned(at):
        return jnp.concatenate([at(x) for x in x_order(sz)], axis=0).T

    def put(c, a, field):
        for half in range(sz.gx):
            out_ref[member_of(sz, part_of(sz, half), c), a] = field[half * sz.planes : (half + 1) * sz.planes]

    for c in range(sz.comps, sz.gy):
        for a in range(2):
            put(c, a, jnp.zeros((sz.zl, sz.lanes), jnp.float32))
    copies[0].wait()
    visc = turned(lambda x: v_ref[x])
    for c in range(sz.comps):
        put(c, 1, visc)
    for c in range(sz.comps):
        copies[1 + c].wait()
        put(c, 0, turned(lambda x: f_ref[c, x]))


def planes_kernel(sz, in_ref, main_ref, *rest):
    edges, scr = rest[:-1], rest[-1]
    for a in range(2):
        for src in range(sz.group):
            scr[pl.ds(row_of(sz, src), sz.planes, stride=sz.group), :] = in_ref[src, a]

        def body(p, n):
            rows = pl.multiple_of(p * sz.group, 8)
            v = scr[pl.ds(rows, n * sz.group), :].reshape(n, sz.group, sz.lanes)
            main_ref[a, pl.ds(p, n)] = swap_blocks(v, sz.gy, sz.yl)

        chunked(0, sz.planes, sz.chunk, body)
        k = 0
        for count in sz.hops:
            if sz.paired:
                lo, hi = 0, sz.planes - count
                odd = odd_slab(sz)
                edges[0][a] = main_ref[a, pl.ds(jnp.where(odd, lo, hi), count)]
                edges[1][a] = main_ref[a, pl.ds(jnp.where(odd, hi, lo), count)]
            elif count < sz.planes:
                edges[k][a] = main_ref[a, 0:count]
                edges[k + 1][a] = main_ref[a, sz.planes - count : sz.planes]
                k += 2


FINE_ARRAYS = 14 + 3 * ITERS + ITERS + 1
COARSE_ARRAYS = 9 + ITERS * CSWEEPS


def basis_kernel(phase, sz, *refs):
    it = iter(refs)
    main_ref = next(it) if phase != 1 else None
    halos = [next(it) for _ in range(2 * len(sz.hops))] if phase != 0 else None
    if phase == 1:
        next(it), next(it)
    if phase == 1 or phase == 0:
        fine_state, coarse_state = next(it), next(it)
    if phase is None:
        fine_state, coarse_state = next(it), next(it)
    gram_out = next(it) if phase != 0 else None
    it = iter([fine_state.at[i] for i in range(FINE_ARRAYS)])
    us = [next(it) for _ in range(ITERS)]
    rhos = [next(it) for _ in range(ITERS + 1)]
    half, cin, cout, cyp, cym, cz, mass, od = (next(it) for _ in range(8))
    sin, sout, syp, sym, szp, szm = (next(it) for _ in range(6))
    sms, sm2s = ([next(it) for _ in range(ITERS)] for _ in range(2))
    it = iter([coarse_state.at[i] for i in range(COARSE_ARRAYS)])
    twice, ccz, cod, kxp, kxm, kyp, kym, kzp, kzm = (next(it) for _ in range(9))
    corrections = [[next(it) for _ in range(CSWEEPS)] for _ in range(ITERS)]

    H, N, W, C = HALO, sz.planes, sz.window, sz.chunk
    Q, QC = W // 2, W // 4

    def run(outer, inner, end, n, body, ref=None):
        cut = min(inner, end)
        lo, hi = {None: (outer, end), 0: (cut, end), 1: (outer, cut)}[phase]
        if lo < hi:
            chunked(lo, hi, n, body)
            if ref is not None and hi == end:
                ref[end] = roll(ref[end - 1], sz.width, ref.ndim - 2)

    plane = (1, sz.rows, sz.lanes)
    lane, sub = lane_iota(plane), sub_iota(plane)
    below = lane < sz.width
    y = lane % sz.width
    last = sub == sz.rows - 1

    def plane_at(a, p):
        if H <= p < H + N:
            return main_ref[a, p - H]
        if sz.paired:
            own, other = (halos[i][a, p if p < H else p - H - N] for i in (0, 1))
            return jnp.where(odd_slab(sz) == (p < H), own, other)
        lo, hi = H, H + N
        for j, count in enumerate(sz.hops):
            if lo - count <= p < lo:
                return halos[2 * j][a, p - lo + count]
            if hi <= p < hi + count:
                return halos[2 * j + 1][a, p - hi]
            lo, hi = lo - count, hi + count

    for a, ref in ((1, half), (0, rhos[0])):

        def place(q, n):
            p = jnp.stack([plane_at(a, q + i) for i in range(n)])
            m = jnp.stack([plane_at(a, W - 1 - q - i) for i in range(n)])
            if a == 1:
                p, m = 0.5 * p, 0.5 * m
            ref[q : q + n, 0] = jnp.where(below, p, roll(m, sz.width, 2))
            ref[q : q + n, 1] = jnp.where(below, roll(p, sz.width, 2), m)

        run(0, H, Q, Q, place, half if a == 1 else None)

    def count_of(*edges):
        return sum(e.astype(jnp.float32) for e in edges)

    def z_faces(cells, faces, inner, size):
        def body(q, n):
            faces[pl.ds(q, n)] = cells[pl.ds(q, n)] + cells[pl.ds(q + 1, n)]

        run(0, inner, size, C // 2, body)

    def close_z(cells, faces, first, step, mass_ref=None):
        if phase == 0:
            return
        for q in range(first, -1, -step):
            outside = ~((cells[q] > 0) & (cells[q + 1] > 0))
            total = faces[q]
            faces[q] = jnp.where(outside, 0.0, total)
            if mass_ref is not None:
                moved = jnp.where(outside, total, 0.0)
                for near in (q, q + 1):
                    if near > 0:
                        mass_ref[near] = mass_ref[near] + moved

    z_faces(half, cz, H, Q)
    edge_out = (sub == 0, last)
    edge_y = y == sz.width - 1

    def fine_coeffs(q, n):
        at, under = pl.ds(q, n), pl.ds(q - 1, n)
        h = [half[at, i] for i in (0, 1)]
        inner = h[0] + h[1]
        outer = [None, jnp.where(last, 0.0, h[1] + roll(h[0], -1, 1))]
        outer[0] = roll(outer[1], 1, 1)
        for i in (0, 1):
            yp = jnp.where(edge_y, 0.0, h[i] + roll(h[i], -1, 2))
            ym = roll(yp, 1, 2)
            m = REACTION + count_of(edge_out[i], edge_y, y == 0) * h[i]
            scale = RELAX / (m + inner + outer[i] + (yp + ym) + (cz[under, i] + cz[at, i]))
            cin[at, i], cout[at, i], cyp[at, i], cym[at, i] = inner, outer[i], yp, ym
            mass[at, i], od[at, i] = m, scale
            sin[at, i], sout[at, i], syp[at, i], sym[at, i] = scale * inner, scale * outer[i], scale * yp, scale * ym

    run(1, H + 1, Q, C // 2, fine_coeffs)
    close_z(half, cz, H - 1, N, mass)

    def fine_z(q, n):
        at = pl.ds(q, n)
        szp[at] = od[at] * cz[at]
        szm[at] = od[at] * cz[pl.ds(q - 1, n)]

    run(1, H + 1, Q, C // 2, fine_z)

    def gather_block(fine, n):
        t = fine.reshape(n, 2, sz.rows, sz.lanes)
        t = t[:, 0] + t[:, 1]
        return t + lane_xor(t, 1)

    def coarse_visc(q, n):
        fine = pl.ds(2 * q, 2 * n)
        twice[pl.ds(q, n)] = 0.5 * gather_block(half[fine, 0] + half[fine, 1], n)

    run(0, H // 2, QC, C // 4, coarse_visc, twice)
    z_faces(twice, ccz, H // 2, QC)
    edge_y2 = y >= sz.width - 2
    outer_coarse = count_of(sub == 0, last, edge_y2, y < 2)

    def coarse_coeffs(q, n):
        at = pl.ds(q, n)
        t = twice[at]
        xp = jnp.where(last, 0.0, t + roll(t, -1, 1))
        yp = jnp.where(edge_y2, 0.0, t + roll(t, -2, 2))
        xm, ym = roll(xp, 1, 1), roll(yp, 2, 2)
        m = 8.0 * REACTION + outer_coarse * t
        scale = RELAX / (m + (xp + xm) + (yp + ym) + (ccz[pl.ds(q - 1, n)] + ccz[at]))
        cod[at] = scale
        kxp[at], kxm[at], kyp[at], kym[at] = scale * xp, scale * xm, scale * yp, scale * ym

    run(1, H // 2 + 1, QC, C // 2, coarse_coeffs)
    close_z(twice, ccz, H // 2 - 1, N // 2)

    def coarse_z(q, n):
        at = pl.ds(q, n)
        kzp[at] = cod[at] * ccz[at]
        kzm[at] = cod[at] * ccz[pl.ds(q - 1, n)]

    run(1, H // 2 + 1, QC, C // 2, coarse_z)

    def fine_beside(ref, q, n, coeffs):
        at, under, over = pl.ds(q, n), pl.ds(q - 1, n), pl.ds(q + 1, n)
        inner, outer, yp, ym, z_over, z_under = coeffs
        out = []
        for i in (0, 1):
            v, w = ref[at, i], ref[at, 1 - i]
            total = inner[at, i] * w + outer[at, i] * roll(w, -1 if i else 1, 1)
            total = total + (z_over(at, under, i) * ref[over, i] + z_under(at, under, i) * ref[under, i])
            out.append(total + (yp[at, i] * roll(v, -1, 2) + ym[at, i] * roll(v, 1, 2)))
        return out

    plain = (cin, cout, cyp, cym, lambda at, under, i: cz[at, i], lambda at, under, i: cz[under, i])
    scaled = (sin, sout, syp, sym, lambda at, under, i: szp[at, i], lambda at, under, i: szm[at, i])

    def fine_apply(ref, q, n):
        at = pl.ds(q, n)
        v = [ref[at, i] for i in (0, 1)]
        fin = cin[at, 0] * (v[0] - v[1])
        fout = cout[at, 1] * (v[1] - roll(v[0], -1, 1))
        fx = (fin - roll(fout, 1, 1), fout - fin)
        out = []
        for i in (0, 1):
            ext = ref[pl.ds(q - 1, n + 2), i]
            flux = cz[pl.ds(q - 1, n + 1), i] * (ext[: n + 1] - ext[1:])
            fy = cyp[at, i] * (v[i] - roll(v[i], -1, 2))
            out.append(mass[at, i] * v[i] + (flux[1:] - flux[:n]) + (fy - roll(fy, 1, 2)) + fx[i])
        return out

    known = H
    for k in range(ITERS):
        outer = H - (HALO - 1 - k * STEP)
        rho, rho_next, u, sm, sm2 = rhos[k], rhos[k + 1], us[k], sms[k], sm2s[k]

        def smooth(q, n):
            sm[pl.ds(q, n)] = od[pl.ds(q, n)] * rho[pl.ds(q, n)]

        known = max(known, H + 1)
        run(outer, known, Q, C // 2, smooth, sm)

        first = corrections[k][0]

        def restricted(q, n):
            fine = pl.ds(2 * q, 2 * n)
            left, right = fine_beside(sm, 2 * q, 2 * n, plain)
            defect = (1.0 - RELAX) * (rho[fine, 0] + rho[fine, 1]) + (left + right)
            first[pl.ds(q, n)] = cod[pl.ds(q, n)] * gather_block(defect, n)

        outer, known = (outer + 1) // 2, (known + 2) // 2
        run(outer, known, QC, C // 4, restricted, first)
        for old, new in zip(corrections[k], corrections[k][1:]):

            def relax(q, n):
                at = pl.ds(q, n)
                v = old[at]
                total = first[at] + (1.0 - RELAX) * v
                total = total + (kzp[at] * old[pl.ds(q + 1, n)] + kzm[at] * old[pl.ds(q - 1, n)])
                total = total + (kxp[at] * roll(v, -1, 1) + kxm[at] * roll(v, 1, 1))
                new[at] = total + (kyp[at] * roll(v, -2, 2) + kym[at] * roll(v, 2, 2))

            outer, known = outer + 1, known + 1
            run(outer, known, QC, C // 2, relax, new)

        def prolonged(q, n):
            c = new[pl.ds(q, n)]
            fine = jnp.stack([c, c], axis=1).reshape(2 * n, sz.rows, sz.lanes)
            for i in (0, 1):
                sm2[pl.ds(2 * q, 2 * n), i] = sm[pl.ds(2 * q, 2 * n), i] + fine

        run(outer, known, QC, C // 4, prolonged)
        if phase is None or phase == (0 if known < QC else 1):
            sm2[Q] = roll(sm2[Q - 1], sz.width, 2)

        def smoothed(q, n):
            at = pl.ds(q, n)
            for i, beside in enumerate(fine_beside(sm2, q, n, scaled)):
                u[at, i] = (1.0 - RELAX) * sm2[at, i] + sm[at, i] + beside

        outer, known = 2 * outer + 1, 2 * known + 1
        run(outer, known, Q, C // 2, smoothed, u)

        def descend(q, n):
            at = pl.ds(q, n)
            for i, image in enumerate(fine_apply(u, q, n)):
                rho_next[at, i] = rho[at, i] - image
                image_of[at, i] = image

        image_of = sm2
        outer, known = outer + 1, known + 1
        run(outer, known, Q, C // 2, descend)

    if phase == 0:
        return
    orders = [((n + 1) // 2, n // 2) for n in range(MOMENTS)]
    zero = jnp.zeros((sz.rows, sz.lanes), jnp.float32)
    sums = [(zero, zero)] * (2 * MOMENTS)
    for q in range(H, Q):
        rv, yv, uv = ([[ref[q, i] for i in (0, 1)] for ref in refs] for refs in (rhos[:ITERS], sm2s, us))
        for place, left in enumerate((rv, yv)):
            for n, (j, k) in enumerate(orders):
                hi, lo = sums[place * MOMENTS + n]
                hi, error = two_sum(hi, left[j][0] * uv[k][0] + left[j][1] * uv[k][1])
                sums[place * MOMENTS + n] = (hi, lo + error)
    wide = -(-len(sums) // 8) * 8

    def rows_of(values, fold):
        rows = [fold(v, axis=0, keepdims=True) for v in values]
        return jnp.concatenate(rows + [jnp.zeros((wide - len(rows), sz.lanes), jnp.float32)], axis=0)

    most = jnp.max(rows_of([jnp.abs(hi) for hi, _ in sums], jnp.max), axis=1, keepdims=True)
    grid = float(sz.rows * sz.lanes) * jnp.broadcast_to(most, (wide, sz.lanes))
    coarse = [(hi + grid[n : n + 1]) - grid[n : n + 1] for n, (hi, _) in enumerate(sums)]
    rest = [(hi - c) + lo for c, (hi, lo) in zip(coarse, sums)]
    line = jnp.zeros((1, sz.lanes), jnp.float32)
    for offset, values in ((0, coarse), (wide, rest)):
        rows = rows_of(values, jnp.sum)
        each = jnp.broadcast_to(jnp.sum(rows, axis=1, keepdims=True), rows.shape)
        here = sub_iota(rows.shape) + offset == lane_iota(rows.shape)
        line = line + jnp.sum(jnp.where(here, each, 0.0), axis=0, keepdims=True)
    gram_out[...] = jnp.broadcast_to(line[None], gram_out.shape)


def combine_kernel(sz, gram_ref, fine_ref, out_ref, scr):
    parts = gram_ref[:, 0, :]
    wide = -(-2 * MOMENTS // 8) * 8
    hi, lo = parts, roll(parts, -wide, 1)
    while hi.shape[0] % 16 == 0:
        n = hi.shape[0] // 2
        hi, error = two_sum(hi[:n], hi[n:])
        lo = lo[:n] + lo[n:] + error
    sum_hi, sum_lo = hi[:1], lo[:1]
    for i in range(1, hi.shape[0]):
        sum_hi, error = two_sum(sum_hi, hi[i : i + 1])
        sum_lo = sum_lo + (lo[i : i + 1] + error)
    lane = lane_iota(sum_hi.shape)

    def entry(n):
        halves = []
        for v in (sum_hi, sum_lo):
            picked = jnp.sum(jnp.where(lane == n, v, 0.0), axis=1, keepdims=True)
            halves.append(jnp.broadcast_to(picked, v.shape))
        return Pair.of(*halves)

    moments = [entry(n) for n in range(2 * MOMENTS)]

    def form(v, moments):
        terms = []
        for n in range(2 * len(v) - 1):
            pairs = [(j, n - j) for j in range(len(v)) if j <= n - j < len(v)]
            weight = total([v[j] * v[k] if j == k else (v[j] * v[k]).twice() for j, k in pairs])
            terms.append(weight * moments[n])
        return total(terms)

    zero = Pair(jnp.zeros_like(sum_hi), jnp.zeros_like(sum_hi))
    one = Pair(jnp.ones_like(sum_hi), jnp.zeros_like(sum_hi))
    res, direction, sol = [one], [one], []
    product = moments[0]
    for i in range(ITERS):
        image = form(direction, moments[MOMENTS:]) if i else moments[MOMENTS]
        alpha = product / image
        steps = [alpha * b for b in direction] if i else [alpha]
        sol = [s + t for s, t in zip(sol, steps)] + steps[-1:]
        res = [r - t for r, t in zip(res, steps)] + [zero]
        res = res[:1] + [r + t for r, t in zip(res[1:-1], steps)] + steps[-1:]
        if i + 1 < ITERS:
            following = form(res, moments)
            beta = following / product
            direction = [a + beta * b for a, b in zip(res, direction)] + res[-1:]
            product = following

    sol = [s.hi.reshape(1, 1, sz.lanes) for s in sol]
    res = [s.hi.reshape(1, 1, sz.lanes) for s in res]
    below = lane_iota((1, sz.rows, sz.lanes)) < sz.width
    for a, (first, weights) in enumerate(((0, sol), (ITERS, res))):

        def body(q, n):
            left, right = (
                sum(w * fine_ref[first + k, pl.ds(HALO + q, n), i] for k, w in enumerate(weights)) for i in (0, 1)
            )
            under = swap_blocks(jnp.where(below, left, roll(right, sz.width, 2)), sz.gy, sz.yl)
            over = swap_blocks(jnp.where(below, roll(left, sz.width, 2), right), sz.gy, sz.yl)
            for i in range(n):
                for p, v in ((q + i, under), (sz.planes - 1 - q - i, over)):
                    row = p * sz.group if isinstance(p, int) else pl.multiple_of(p * sz.group, 8)
                    scr[pl.ds(row, sz.group), :] = v[i]

        chunked(0, sz.planes // 2, sz.chunk // 2, body)
        for dest in range(sz.group):
            out_ref[dest, a] = scr[pl.ds(row_of(sz, dest), sz.planes, stride=sz.group), :]


def unpack_kernel(sz, in_ref, sol_ref, res_ref):
    for a, out in ((0, sol_ref), (1, res_ref)):
        for c in range(sz.comps):
            halves = [in_ref[member_of(sz, part_of(sz, half), c), a] for half in range(sz.gx)]
            turned = jnp.concatenate(halves, axis=0).T
            for i, x in enumerate(x_order(sz)):
                out[c, x] = turned[i * sz.yl : (i + 1) * sz.yl]


def call(kernel, sz, ins, outs, scratch=(), name=None, sems=0, alias={}):
    outs = [jax.ShapeDtypeStruct(s, jnp.float32) for s in outs]
    own = [a.shape for i, a in enumerate(ins) if i not in alias]
    held = sum(math.prod(s) for s in own + [o.shape for o in outs] + list(scratch))
    scratch = [pltpu.VMEM(s, jnp.float32) for s in scratch]
    return pl.pallas_call(
        functools.partial(kernel, sz),
        in_specs=[pl.BlockSpec(memory_space=pltpu.HBM if sems else pltpu.VMEM)] * len(ins),
        out_specs=[pl.BlockSpec(memory_space=pltpu.VMEM)] * len(outs),
        out_shape=outs,
        scratch_shapes=scratch + ([pltpu.SemaphoreType.DMA((sems,))] if sems else []),
        compiler_params=pltpu.CompilerParams(vmem_limit_bytes=4 * held + 3 * 2**20),
        input_output_aliases=alias,
        name=name,
    )(*ins)


def shards(mesh, forcing, viscosity):
    comps, xl, yl, zl = forcing.shape
    sz = Sizes(mesh, comps, xl, yl, zl)
    N, W = sz.planes, sz.window
    plane = (sz.rows, sz.lanes)
    group_shape = (sz.group, 2, N, sz.lanes)
    arrays = [pltpu.with_memory_space_constraint(a, pltpu.HBM) for a in (forcing, viscosity)]
    (packed,) = call(
        pack_kernel, sz, arrays, [group_shape], [a.shape for a in arrays], name="pack", sems=1 + sz.comps
    )
    packed = lax.all_to_all(packed, GROUP, 0, 0)
    edge_shapes = [(2, c) + plane for c in sz.hops if c < N for _ in range(2)]
    main, *edges = call(
        planes_kernel, sz, [packed], [(2, N) + plane] + edge_shapes, [(N * sz.group, sz.lanes)], name="planes"
    )
    halos = []
    if sz.paired:
        halos = [swapped_pairs(edge, sz, first) for first, edge in reversed(list(enumerate(edges)))][::-1]
    for j, count in enumerate([] if sz.paired else sz.hops):
        first, last = (edges.pop(0), edges.pop(0)) if count < N else (main, main)
        halos += [shifted(last, sz, j + 1), shifted(first, sz, -(j + 1))]
    devices = sz.group * sz.gz
    state = [(FINE_ARRAYS, W // 2 + 1, 2) + plane, (COARSE_ARRAYS, W // 4 + 1) + plane]
    gram_shape = (devices, 1, sz.lanes)
    if sum(math.prod(shape) for shape in state) <= STATE_LIMIT:
        held = call(functools.partial(basis_kernel, 0), sz, [main], state, name="inner")
        alias = {len(halos): 0, len(halos) + 1: 1}
        outer = functools.partial(basis_kernel, 1)
        fine, _, gram = call(outer, sz, halos + list(held), state + [gram_shape], name="outer", alias=alias)
    else:
        whole = functools.partial(basis_kernel, None)
        fine, _, gram = call(whole, sz, [main] + halos, state + [gram_shape], name="basis")
    gram = lax.all_to_all(gram, ("gx", "gy", "gz"), 0, 0)
    (mixed,) = call(
        combine_kernel, sz, [gram, fine], [group_shape], [(N * sz.group, sz.lanes)], name="combine"
    )
    mixed = lax.all_to_all(mixed, GROUP, 0, 0)
    return tuple(call(unpack_kernel, sz, [mixed], [forcing.shape, forcing.shape], name="unpack"))


def solution(mesh):
    spec = P(None, "gx", "gy", "gz")
    return jax.shard_map(
        functools.partial(shards, dict(mesh.shape)),
        mesh=mesh,
        in_specs=(spec, P("gx", "gy", "gz")),
        out_specs=(spec, spec),
        check_vma=False,
    )
```
